16 devices in a mesh: dz: 2 (over z), dy: 2 (over y), dx: 4 (over x, core).
Axes of the slice: x: 2, y: 2, z: 2, core: 2. Of those that a mesh axis runs over, the one named last changes fastest.
Arguments:
- act_one: bfloat16 [32768, 768], P(('dz', 'dy', 'dx'))
- pre_one: bfloat16 [32768, 3072], P(('dz', 'dy', 'dx'))
- act_two: bfloat16 [32768, 768], P(('dz', 'dy', 'dx'))
- pre_two: bfloat16 [32768, 3072], P(('dz', 'dy', 'dx'))
- grad_out: bfloat16 [32768, 768], P(('dz', 'dy', 'dx'))
- w_in_two: bfloat16 [768, 3072], replicated
- w_out_one: bfloat16 [3072, 768], replicated
- w_out_two: bfloat16 [3072, 768], replicated
Outputs:
- output: float32 [9437184], P(('dx', 'dy', 'dz'))
All inputs are finite; a program needn't handle non-finite values.
Results may differ from the reference program's by a relative error of at most 0.00159.
Values are sent between devices in bfloat16 or wider.
A program may use at most 1 GiB of HBM per device.

```python
import jax
import jax.numpy as jnp
from jax import lax

D = 768
FF = 3072
TOKENS_DEV = 2048
N_DEVICES = 16
N_MICRO = 2


def setup_inputs(seed: int = 0) -> dict:
    key_list = jax.random.split(jax.random.key(seed), 8)
    row_count = N_DEVICES * TOKENS_DEV
    grad_scale = (N_DEVICES * TOKENS_DEV) ** -0.5
    drawn = {
        'act_one': jax.random.normal(key_list[0], (row_count, D), jnp.float32),
        'pre_one': jax.random.normal(key_list[1], (row_count, FF), jnp.float32),
        'act_two': jax.random.normal(key_list[2], (row_count, D), jnp.float32),
        'pre_two': jax.random.normal(key_list[3], (row_count, FF), jnp.float32),
        'grad_out': jax.random.normal(key_list[4], (row_count, D), jnp.float32) * grad_scale,
        'w_in_two': jax.random.normal(key_list[5], (D, FF), jnp.float32) * D ** -0.5,
        'w_out_one': jax.random.normal(key_list[6], (FF, D), jnp.float32) * FF ** -0.5,
        'w_out_two': jax.random.normal(key_list[7], (FF, D), jnp.float32) * FF ** -0.5,
    }
    return {key_name: drawn_val.astype(jnp.bfloat16) for key_name, drawn_val in drawn.items()}


def gelu_pair(pre):
    pre_wide = pre.astype(jnp.float32)
    hidden, pull_back = jax.vjp(jax.nn.gelu, pre_wide)
    return hidden, pull_back(jnp.ones_like(pre_wide))[0]


def micro_grads(act_one, pre_one, act_two, pre_two, grad_out, w_in_two, w_out_one, w_out_two):
    hid_two, slope_two = gelu_pair(pre_two)
    hid_two = hid_two.astype(jnp.bfloat16)
    g_out_two = jnp.dot(hid_two.T, grad_out, preferred_element_type=jnp.float32).astype(jnp.bfloat16)
    d_hid_two = jnp.dot(grad_out, w_out_two.T, preferred_element_type=jnp.float32)
    d_pre_two = (d_hid_two * slope_two).astype(jnp.bfloat16)
    g_in_two = jnp.dot(act_two.T, d_pre_two, preferred_element_type=jnp.float32).astype(jnp.bfloat16)
    d_back_two = jnp.dot(d_pre_two, w_in_two.T, preferred_element_type=jnp.float32)
    d_act_two = (grad_out.astype(jnp.float32) + d_back_two).astype(jnp.bfloat16)
    hid_one, slope_one = gelu_pair(pre_one)
    hid_one = hid_one.astype(jnp.bfloat16)
    g_out_one = jnp.dot(hid_one.T, d_act_two, preferred_element_type=jnp.float32).astype(jnp.bfloat16)
    d_hid_one = jnp.dot(d_act_two, w_out_one.T, preferred_element_type=jnp.float32)
    d_pre_one = (d_hid_one * slope_one).astype(jnp.bfloat16)
    g_in_one = jnp.dot(act_one.T, d_pre_one, preferred_element_type=jnp.float32).astype(jnp.bfloat16)
    return (g_out_two, g_in_two, g_out_one, g_in_one)


def reference(act_one, pre_one, act_two, pre_two, grad_out, w_in_two, w_out_one, w_out_two):
    micro_rows = TOKENS_DEV // N_MICRO
    batch_count = N_DEVICES * N_MICRO
    stacked = tuple(array_in.reshape(batch_count, micro_rows, array_in.shape[1]) for array_in in (act_one, pre_one, act_two, pre_two, grad_out))

    def scan_step(running, micro_slab):
        micro_out = micro_grads(*micro_slab, w_in_two, w_out_one, w_out_two)
        return tuple(run_sum + grad_piece.astype(jnp.float32) for run_sum, grad_piece in zip(running, micro_out)), None

    zero_sums = (jnp.zeros((FF, D), jnp.float32), jnp.zeros((D, FF), jnp.float32), jnp.zeros((FF, D), jnp.float32), jnp.zeros((D, FF), jnp.float32))
    grad_sums, _ = lax.scan(scan_step, zero_sums, stacked)
    return jnp.concatenate([grad_piece.reshape(-1) for grad_piece in grad_sums])
```

```python
import math

import jax
import jax.numpy as jnp
from jax import lax
from jax.experimental import pallas as pl
from jax.experimental.pallas import tpu as pltpu
from jax.sharding import PartitionSpec as P

MESH = pl.DeviceIdType.MESH
D = 768
FF = 3072
ROWS = 2048
MICRO = 1024
UNITS = 6
WIDE = 512
STEPS = 2 * UNITS
SLOTS = 6
LAG1, LAG2, LAG3 = 2, 4, 6
N_SUM = LAG3 + 1
PARTS = (('yzx', 256), ('zyx', 256), ('xyz', 128), ('xzy', 128))
ROOT = math.sqrt(2.0 / math.pi)
CUBE = 0.044715


def gelu_pair(val):
    sq = val * val
    tan = jnp.tanh(val * (sq * (ROOT * CUBE) + ROOT))
    cdf = 0.5 * tan + 0.5
    bump = val * (cdf * (1.0 - cdf))
    return val * cdf, cdf + bump * (sq * (6.0 * ROOT * CUBE) + 2.0 * ROOT)


def part_layout():
    start = 0
    table = []
    for order, rows in PARTS:
        table.append((order, start, rows))
        start += rows
    return table


def landing_dims(order, stage):
    done = order[:stage + 1]
    return (1 if 'y' in done else 2), (1 if 'z' in done else 2)


def kernel(a1_hbm, z1_hbm, a2_hbm, z2_hbm, g_hbm, wi_hbm, wo1_hbm, wo2_hbm, out_ref,
           dy_v, x_v, acc_v, z_v, h_v, dz_v, wo_v, wi_v, big, drecv, *rest):
    landings = rest[:12]
    isem, fsem, dsend_sem, drecv_sem, send_sem, recv_sem = rest[12:]
    f32, bf16 = jnp.float32, jnp.bfloat16
    dx, y, z = lax.axis_index('dx'), lax.axis_index('dy'), lax.axis_index('dz')
    x, core = dx // 2, dx % 2
    peers = {'x': {'dx': (dx + 2) % 4}, 'y': {'dy': 1 - y}, 'z': {'dz': 1 - z}, 'c': {'dx': dx + 1 - 2 * core}}

    barrier = pltpu.get_barrier_semaphore()
    for name in 'xyzc':
        pl.semaphore_signal(barrier, inc=1, device_id=peers[name], device_id_type=MESH)

    load_g = pltpu.make_async_copy(g_hbm, dy_v, isem.at[0])
    load_2 = pltpu.make_async_copy(a2_hbm, x_v.at[0], isem.at[1])
    load_1 = pltpu.make_async_copy(a1_hbm, x_v.at[1], isem.at[2])

    def fetch(unit, slot, z_hbm, wo_hbm, with_wi):
        copies = []
        for quarter in range(4):
            cols = pl.ds(pl.multiple_of(quarter * 768 + unit * 128, 128), 128)
            put = pl.ds(quarter * 128, 128)
            copies.append(pltpu.make_async_copy(z_hbm.at[:, cols], z_v.at[slot, :, put], fsem.at[slot, quarter]))
            copies.append(pltpu.make_async_copy(wo_hbm.at[cols, :], wo_v.at[slot, put, :], fsem.at[slot, 4 + quarter]))
            if with_wi:
                copies.append(pltpu.make_async_copy(wi_hbm.at[:, cols], wi_v.at[slot, :, put], fsem.at[slot, 8 + quarter]))
        return copies

    def fetch_start(step):
        @pl.when(step < UNITS)
        def _():
            for cp in fetch(step, step % 2, z2_hbm, wo2_hbm, True):
                cp.start()

        @pl.when((step >= UNITS) & (step < STEPS))
        def _():
            for cp in fetch(step - UNITS, step % 2, z1_hbm, wo1_hbm, False):
                cp.start()

    def fetch_wait(step):
        @pl.when(step < UNITS)
        def _():
            for cp in fetch(step, step % 2, z2_hbm, wo2_hbm, True):
                cp.wait()

        @pl.when((step >= UNITS) & (step < STEPS))
        def _():
            for cp in fetch(step - UNITS, step % 2, z1_hbm, wo1_hbm, False):
                cp.wait()

    load_g.start()
    fetch_start(0)
    load_2.start()
    load_1.start()
    pl.semaphore_wait(barrier, 4)
    load_g.wait()

    def d2d_copy(unit):
        return pltpu.make_async_remote_copy(src_ref=big.at[N_SUM], dst_ref=drecv.at[unit % 2], send_sem=dsend_sem.at[0],
                                            recv_sem=drecv_sem.at[unit % 2], device_id=peers['c'], device_id_type=MESH)

    layout = part_layout()

    def views(order, stage, start, rows, unit):
        slot = unit % N_SUM
        done, axis = order[:stage], order[stage]
        keep_y = pl.ds(y, 1) if ('y' in done or axis == 'y') else pl.ds(0, 2)
        keep_z = pl.ds(z, 1) if ('z' in done or axis == 'z') else pl.ds(0, 2)
        away_y = pl.ds(1 - y, 1) if axis == 'y' else keep_y
        away_z = pl.ds(1 - z, 1) if axis == 'z' else keep_z
        away = big.at[slot, away_y, away_z, pl.ds(start, rows), :]
        return away, keep_y, keep_z

    def stage_copy(idx, stage, unit):
        order, start, rows = layout[idx]
        away, _, _ = views(order, stage, start, rows, unit)
        slot = unit % SLOTS
        return pltpu.make_async_remote_copy(src_ref=away, dst_ref=landings[idx * 3 + stage].at[slot],
                                            send_sem=send_sem.at[idx * 3 + stage, slot], recv_sem=recv_sem.at[idx * 3 + stage, slot],
                                            device_id=peers[order[stage]], device_id_type=MESH)

    def stage_roles(idx, stage, unit):
        order = layout[idx][0]
        owner = x == unit // UNITS
        if order[stage] == 'x':
            return x != unit // UNITS, owner
        if 'x' in order[:stage]:
            return owner, owner
        return None, None

    def guarded(cond, body):
        if cond is None:
            body()
        else:
            pl.when(cond)(body)

    def stage_send(idx, stage, unit):
        send_if, _ = stage_roles(idx, stage, unit)
        guarded(send_if, lambda: stage_copy(idx, stage, unit).start())

    def stage_take(idx, stage, unit):
        order, start, rows = layout[idx]
        send_if, recv_if = stage_roles(idx, stage, unit)
        ny, nz = landing_dims(order, stage)
        sum_slot, slot = unit % N_SUM, unit % SLOTS
        land = landings[idx * 3 + stage]
        done = order[:stage + 1]

        def take():
            stage_copy(idx, stage, unit).wait_recv()
            for iy in range(ny):
                for iz in range(nz):
                    at_y = y if 'y' in done else iy
                    at_z = z if 'z' in done else iz

                    def chunk(k, carry):
                        offset = pl.multiple_of(k * 64, 64)
                        here = (sum_slot, at_y, at_z, pl.ds(start + offset, 64), slice(None))
                        big[here] = big[here] + land[slot, iy, iz, pl.ds(offset, 64), :]
                        return carry

                    lax.fori_loop(0, rows // 64, chunk, 0)

        guarded(send_if, lambda: stage_copy(idx, stage, unit).wait_send())
        guarded(recv_if, take)

    def chip_sum(unit):
        cp = d2d_copy(unit)
        cp.wait()
        sum_slot = unit % N_SUM
        for iy in range(2):
            for iz in range(2):
                def chunk(k, carry):
                    here = pl.ds(pl.multiple_of(k * 64, 64), 64)
                    big[sum_slot, iy, iz, here, :] = big[sum_slot, iy, iz, here, :] + drecv[unit % 2, iy, iz, here, :]
                    return carry

                lax.fori_loop(0, 768 // 64, chunk, 0)

    def finish(unit):
        sum_slot, pos = unit % N_SUM, unit % UNITS

        @pl.when((x == unit // UNITS) & (core == 0))
        def _():
            for j in range(6):
                out_ref[pl.ds(768 * pos + j, 128, stride=6), :] = big[sum_slot, y, z, pl.ds(128 * j, 128), :]

        @pl.when((x == unit // UNITS) & (core == 1))
        def _():
            for q in range(4):
                out_ref[pl.ds(6 * q + pos, 192, stride=24), :] = big[sum_slot, y, z, pl.ds(192 * q, 192), :]

    def step_body(step, carry):
        slot = step % 2
        phase = jnp.where(step >= UNITS, 1, 0)

        @pl.when(step < STEPS)
        def _():
            fetch_wait(step)
            fetch_start(step + 1)

            def tile(t, c):
                rows = pl.ds(pl.multiple_of(t * 256, 256), 256)
                hid, slope = gelu_pair(z_v[slot, rows, :].astype(f32))
                h_v[rows, :] = hid.astype(bf16)
                dh = lax.dot_general(dy_v[rows, :], wo_v[slot], (((1,), (1,)), ((), ())), preferred_element_type=f32)
                dz_v[rows, :] = (dh * slope).astype(bf16)
                return c

            lax.fori_loop(0, ROWS // 256, tile, 0)

        @pl.when((step >= 1) & (step <= STEPS))
        def _():
            unit = step - 1
            chip_sum(unit)
            for idx in range(4):
                stage_send(idx, 0, unit)

        for lag, stage in ((LAG1, 0), (LAG2, 1), (LAG3, 2)):
            unit = step - 1 - lag

            @pl.when((unit >= 0) & (unit < STEPS))
            def _(unit=unit, stage=stage):
                for idx in range(4):
                    stage_take(idx, stage, unit)
                    if stage < 2:
                        stage_send(idx, stage + 1, unit)
                if stage == 2:
                    finish(unit)

        @pl.when(step < STEPS)
        def _():
            own = step % N_SUM
            slot_a = jnp.where(core == 0, own, N_SUM)
            slot_b = jnp.where(core == 0, N_SUM, own)

            def grad_a(nb, c):
                cols = pl.ds(pl.multiple_of(nb * 256, 256), 256)
                total = None
                for m in range(2):
                    rows = pl.ds(m * MICRO, MICRO)
                    got = lax.dot_general(h_v[rows, :], dy_v[rows, cols], (((0,), (0,)), ((), ())), preferred_element_type=f32)
                    got = got.astype(bf16).astype(f32)
                    total = got if total is None else total + got
                for q in range(4):
                    for j in range(2):
                        big[slot_a, q // 2, q % 2, pl.ds(pl.multiple_of((2 * nb + j) * 128, 128), 128), :] = total[128 * q:128 * q + 128, 128 * j:128 * j + 128]
                return c

            lax.fori_loop(0, 3, grad_a, 0)
            pl.when(core == 1)(lambda: d2d_copy(step).start())

            @pl.when(step == 0)
            def _():
                load_2.wait()

            @pl.when(step == UNITS)
            def _():
                load_1.wait()

            def grad_b(nb, c):
                cols = pl.ds(pl.multiple_of(nb * 256, 256), 256)
                total = None
                for m in range(2):
                    rows = pl.ds(m * MICRO, MICRO)
                    got = lax.dot_general(x_v[phase, rows, :], dz_v[rows, cols], (((0,), (0,)), ((), ())), preferred_element_type=f32)
                    got = got.astype(bf16).astype(f32)
                    total = got if total is None else total + got
                for q in range(4):
                    for j in range(2):
                        big[slot_b, q // 2, q % 2, pl.ds(pl.multiple_of((2 * nb + j) * 192, 64), 192), :] = total[192 * q:192 * q + 192, 128 * j:128 * j + 128]
                return c

            lax.fori_loop(0, 2, grad_b, 0)
            pl.when(core == 0)(lambda: d2d_copy(step).start())

        @pl.when(step < UNITS)
        def _():
            def back(t, c):
                rows = pl.ds(pl.multiple_of(t * 512, 512), 512)
                add = lax.dot_general(dz_v[rows, :], wi_v[slot], (((1,), (1,)), ((), ())), preferred_element_type=f32)

                @pl.when(step == 0)
                def _():
                    acc_v[rows, :] = add

                @pl.when(step > 0)
                def _():
                    acc_v[rows, :] = acc_v[rows, :] + add
                return c

            lax.fori_loop(0, ROWS // 512, back, 0)

        @pl.when(step == UNITS - 1)
        def _():
            def close(t, c):
                rows = pl.ds(pl.multiple_of(t * 32, 32), 32)
                dy_v[rows, :] = (dy_v[rows, :].astype(f32) + acc_v[rows, :]).astype(bf16)
                return c

            lax.fori_loop(0, ROWS // 32, close, 0)

        return carry

    lax.fori_loop(0, STEPS + 1 + LAG3, step_body, 0)


def solution(mesh):
    row_spec = P(('dz', 'dy', 'dx'), None)
    full_spec = P(None, None)

    def per_device(*arrays):
        f32, bf16 = jnp.float32, jnp.bfloat16
        landings = []
        for order, rows in PARTS:
            for stage in range(3):
                ny, nz = landing_dims(order, stage)
                landings.append(pltpu.VMEM((SLOTS, ny, nz, rows, 128), f32))
        out = pl.pallas_call(
            kernel,
            out_shape=jax.ShapeDtypeStruct((4608, 128), f32),
            in_specs=[pl.BlockSpec(memory_space=pl.ANY)] * 8,
            out_specs=pl.BlockSpec(memory_space=pltpu.VMEM),
            scratch_shapes=[
                pltpu.VMEM((ROWS, D), bf16),
                pltpu.VMEM((2, ROWS, D), bf16),
                pltpu.VMEM((ROWS, D), f32),
                pltpu.VMEM((2, ROWS, WIDE), bf16),
                pltpu.VMEM((ROWS, WIDE), bf16),
                pltpu.VMEM((ROWS, WIDE), bf16),
                pltpu.VMEM((2, WIDE, D), bf16),
                pltpu.VMEM((2, D, WIDE), bf16),
                pltpu.VMEM((N_SUM + 1, 2, 2, 768, 128), f32),
                pltpu.VMEM((2, 2, 2, 768, 128), f32),
                *landings,
                pltpu.SemaphoreType.DMA((3,)),
                pltpu.SemaphoreType.DMA((2, 12)),
                pltpu.SemaphoreType.DMA((1,)),
                pltpu.SemaphoreType.DMA((2,)),
                pltpu.SemaphoreType.DMA((12, SLOTS)),
                pltpu.SemaphoreType.DMA((12, SLOTS)),
            ],
            compiler_params=pltpu.CompilerParams(collective_id=0, has_side_effects=True, vmem_limit_bytes=67043328),
        )(*arrays)
        return out.reshape(-1)

    return jax.shard_map(per_device, mesh=mesh, in_specs=(row_spec,) * 5 + (full_spec,) * 3, out_specs=P(('dx', 'dy', 'dz')), check_vma=False)
```

```python
import math

import jax
import jax.numpy as jnp
from jax import lax
from jax.experimental import pallas as pl
from jax.experimental.pallas import tpu as pltpu
from jax.sharding import PartitionSpec as P

MESH = pl.DeviceIdType.MESH
D = 768
FF = 3072
ROWS = 2048
MICRO = 1024
UNITS = 6
WIDE = 512
STEPS = 2 * UNITS
SLOTS = 6
ORDERS = ('yzx', 'zyx', 'xyz', 'xzy', 'wyzx', 'wzyx')
TAKES = {
    (0, 0): (7, 11, 15, 19, 23, 27, 37, 41, 47, 53, 59, 65),
    (0, 1): (11, 15, 19, 25, 29, 33, 49, 55, 62, 68, 71, 73),
    (0, 2): (19, 23, 33, 41, 45, 47, 49, 58, 62, 68, 72, 75),
    (1, 0): (9, 13, 17, 21, 29, 37, 37, 37, 41, 45, 52, 55),
    (1, 1): (13, 17, 21, 25, 35, 47, 47, 49, 54, 60, 66, 69),
    (1, 2): (17, 21, 25, 29, 43, 58, 58, 66, 69, 71, 73, 74),
    (2, 0): (9, 13, 17, 21, 25, 29),
    (2, 1): (13, 17, 21, 25, 31, 37),
    (2, 2): (17, 21, 25, 31, 37, 49),
    (2, 3): (25, 33, 39, 43, 48, 51),
}
FINISH = (25, 33, 39, 43, 48, 58, 58, 66, 69, 71, 73, 75)
N_SUM = 8
TICKS = 76
ROWS_ONE = (192, 192, 96, 96, 96, 96)
ROWS_TWO = (320, 320, 64, 64, 0, 0)
ROOT = math.sqrt(2.0 / math.pi)
CUBE = 0.044715


def gelu_pair(val):
    sq = val * val
    tan = jnp.tanh(val * (sq * (ROOT * CUBE) + ROOT))
    cdf = 0.5 * tan + 0.5
    bump = val * (cdf * (1.0 - cdf))
    return val * cdf, cdf + bump * (sq * (6.0 * ROOT * CUBE) + 2.0 * ROOT)


def landing_dims(order, stage):
    done = order[:stage + 1]
    return (1 if 'y' in done else 2), (1 if 'z' in done else 2)


def stage_list():
    return [(idx, stage) for idx, order in enumerate(ORDERS) for stage in range(len(order))]


STAGES = stage_list()


def kernel(a1_hbm, z1_hbm, a2_hbm, z2_hbm, g_hbm, wi_hbm, wo1_hbm, wo2_hbm, out_ref,
           dy_v, x_v, acc_v, z_v, hnew_v, h_v, slope_v, dz_v, wo_v, wi_v, big, drecv, *rest):
    landings = dict(zip(STAGES, rest[:len(STAGES)]))
    isem, zsem, osem, wsem, dsend_sem, drecv_sem, send_sem, recv_sem = rest[len(STAGES):]
    f32, bf16 = jnp.float32, jnp.bfloat16
    dx, y, z = lax.axis_index('dx'), lax.axis_index('dy'), lax.axis_index('dz')
    x, core = dx // 2, dx % 2
    peers = {'x': {'dx': (dx + 2) % 4}, 'y': {'dy': 1 - y}, 'z': {'dz': 1 - z}, 'c': {'dx': dx + 1 - 2 * core}}
    peers['w'] = peers['x']

    barrier = pltpu.get_barrier_semaphore()
    for name in 'xyzc':
        pl.semaphore_signal(barrier, inc=1, device_id=peers[name], device_id_type=MESH)

    load_g = pltpu.make_async_copy(g_hbm, dy_v, isem.at[0])
    load_2 = pltpu.make_async_copy(a2_hbm, x_v, isem.at[1])
    load_1 = pltpu.make_async_copy(a1_hbm, x_v, isem.at[2])

    def columns(unit, quarter):
        return pl.ds(pl.multiple_of(quarter * 768 + unit * 128, 128), 128), pl.ds(quarter * 128, 128)

    def z_copies(unit, hbm):
        pairs = [columns(unit, q) for q in range(4)]
        return [pltpu.make_async_copy(hbm.at[:, get], z_v.at[:, put], zsem.at[q]) for q, (get, put) in enumerate(pairs)]

    def wo_copies(unit, hbm):
        pairs = [columns(unit, q) for q in range(4)]
        return [pltpu.make_async_copy(hbm.at[get, :], wo_v.at[put, :], osem.at[q]) for q, (get, put) in enumerate(pairs)]

    def wi_copies(unit):
        pairs = [columns(unit, q) for q in range(4)]
        return [pltpu.make_async_copy(wi_hbm.at[:, get], wi_v.at[:, put], wsem.at[q]) for q, (get, put) in enumerate(pairs)]

    def by_phase(step, make, action):
        @pl.when(step < UNITS)
        def _():
            for cp in make(step, 0):
                action(cp)

        @pl.when((step >= UNITS) & (step < STEPS))
        def _():
            for cp in make(step - UNITS, 1):
                action(cp)

    def z_make(unit, phase):
        return z_copies(unit, z1_hbm if phase else z2_hbm)

    def wo_make(unit, phase):
        return wo_copies(unit, wo1_hbm if phase else wo2_hbm)

    def start(cp):
        cp.start()

    def wait(cp):
        cp.wait()

    for cp in z_copies(0, z2_hbm):
        cp.start()
    for cp in wo_copies(0, wo2_hbm):
        cp.start()
    load_g.start()
    load_2.start()
    for cp in wi_copies(0):
        cp.start()

    def gelu_rows(start, count):
        for k in range(count // 32):
            rows = pl.ds(pl.multiple_of(start + k * 32, 32), 32)
            hid, slope = gelu_pair(z_v[rows, :].astype(f32))
            hnew_v[rows, :] = hid.astype(bf16)
            slope_v[rows, :] = slope

    for cp in z_copies(0, z2_hbm):
        cp.wait()

    def first_gelu(t, c):
        gelu_rows(t * 128, 128)
        return c

    lax.fori_loop(0, ROWS // 128, first_gelu, 0)
    for cp in z_copies(1, z2_hbm):
        cp.start()
    load_g.wait()
    pl.semaphore_wait(barrier, 4)

    def d2d_copy(unit):
        return pltpu.make_async_remote_copy(src_ref=big.at[N_SUM], dst_ref=drecv.at[unit % 2], send_sem=dsend_sem.at[0],
                                            recv_sem=drecv_sem.at[unit % 2], device_id=peers['c'], device_id_type=MESH)

    def placed(phase):
        sizes = (ROWS_ONE, ROWS_TWO)[phase]
        starts = [sum(sizes[:k]) for k in range(len(sizes))]
        return list(zip(starts, sizes))

    def stage_copy(idx, stage, unit, phase):
        order = ORDERS[idx]
        first, rows = placed(phase)[idx]
        done, axis = order[:stage], order[stage]
        at_y = pl.ds(1 - y, 1) if axis == 'y' else pl.ds(y, 1) if 'y' in done else pl.ds(0, 2)
        at_z = pl.ds(1 - z, 1) if axis == 'z' else pl.ds(z, 1) if 'z' in done else pl.ds(0, 2)
        slot, sem = unit % SLOTS, STAGES.index((idx, stage))
        return pltpu.make_async_remote_copy(src_ref=big.at[unit % N_SUM, at_y, at_z, pl.ds(first, rows), :],
                                            dst_ref=landings[idx, stage].at[slot, :, :, pl.ds(0, rows), :],
                                            send_sem=send_sem.at[sem, slot], recv_sem=recv_sem.at[sem, slot],
                                            device_id=peers[axis], device_id_type=MESH)

    def roles(idx, stage, phase):
        order = ORDERS[idx]
        if order[stage] == 'w':
            return x == phase, x != phase
        if order[stage] == 'x':
            return x != phase, x == phase
        done = order[:stage]
        if 'x' in done:
            return x == phase, x == phase
        if 'w' in done:
            return x != phase, x != phase
        return None, None

    def guarded(cond, body):
        if cond is None:
            body()
        else:
            pl.when(cond)(body)

    def stage_send(idx, stage, unit, phase):
        guarded(roles(idx, stage, phase)[0], lambda: stage_copy(idx, stage, unit, phase).start())

    def stage_take(idx, stage, unit, phase):
        order = ORDERS[idx]
        first, rows = placed(phase)[idx]
        send_if, recv_if = roles(idx, stage, phase)
        ny, nz = landing_dims(order, stage)
        land, done = landings[idx, stage], order[:stage + 1]
        back = order[0] == 'w' and order[stage] == 'x'
        size = max(n for n in (96, 80, 64, 48, 32) if rows % n == 0)

        def take():
            stage_copy(idx, stage, unit, phase).wait_recv()
            for iy in range(ny):
                for iz in range(nz):
                    at_y = y if 'y' in done else iy
                    at_z = z if 'z' in done else iz

                    def chunk(k, carry):
                        offset = pl.multiple_of(k * size, 16)
                        here = (unit % N_SUM, at_y, at_z, pl.ds(first + offset, size), slice(None))
                        got = land[unit % SLOTS, iy, iz, pl.ds(offset, size), :]
                        big[here] = got if back else big[here] + got
                        return carry

                    lax.fori_loop(0, rows // size, chunk, 0)

        guarded(send_if, lambda: stage_copy(idx, stage, unit, phase).wait_send())
        guarded(recv_if, take)

    def part_list(phase):
        return [idx for idx in range(len(ORDERS)) if placed(phase)[idx][1]]

    def chip_sum(unit):
        d2d_copy(unit).wait()
        for iy in range(2):
            for iz in range(2):
                def chunk(k, carry):
                    here = pl.ds(pl.multiple_of(k * 128, 128), 128)
                    big[unit % N_SUM, iy, iz, here, :] = big[unit % N_SUM, iy, iz, here, :] + drecv[unit % 2, iy, iz, here, :]
                    return carry

                lax.fori_loop(0, 768 // 128, chunk, 0)
        for phase in range(2):
            @pl.when(unit // UNITS == phase)
            def _(phase=phase):
                for idx in part_list(phase):
                    stage_send(idx, 0, unit, phase)

    def finish(unit):
        sum_slot, pos = unit % N_SUM, unit % UNITS

        @pl.when((x == unit // UNITS) & (core == 0))
        def _():
            for j in range(6):
                out_ref[pl.ds(768 * pos + j, 128, stride=6), :] = big[sum_slot, y, z, pl.ds(128 * j, 128), :]

        @pl.when((x == unit // UNITS) & (core == 1))
        def _():
            for q in range(4):
                out_ref[pl.ds(6 * q + pos, 192, stride=24), :] = big[sum_slot, y, z, pl.ds(192 * q, 192), :]

    def reached(tick, row):
        total = jnp.int32(0)
        for value in row:
            total = total + jnp.where(tick >= value, 1, 0)
        return total

    def run_ticks(tick, seen):
        now = []
        for place, (key, row) in enumerate(sorted(TAKES.items())):
            group, stage = key
            count = reached(tick, row)

            def one(unit, carry):
                for phase in range(2):
                    members = [i for i in (2 * group, 2 * group + 1) if placed(phase)[i][1]]
                    if not members:
                        continue

                    @pl.when(unit // UNITS == phase)
                    def _(phase=phase, members=members):
                        for idx in members:
                            stage_take(idx, stage, unit, phase)
                            if stage + 1 < len(ORDERS[idx]):
                                stage_send(idx, stage + 1, unit, phase)
                return carry

            lax.fori_loop(seen[place], count, one, 0)
            now.append(count)
        count = reached(tick, FINISH)

        def last(unit, carry):
            finish(unit)
            return carry

        lax.fori_loop(seen[-1], count, last, 0)
        now.append(count)
        return tuple(now)

    def body(tick, seen):
        step, part = tick // 4, tick % 4
        live = step < STEPS

        @pl.when(live & (part == 0))
        def _():
            by_phase(step, wo_make, wait)

            def tile(t, c):
                rows = pl.ds(pl.multiple_of(t * 256, 256), 256)
                h_v[rows, :] = hnew_v[rows, :]
                dh = lax.dot_general(dy_v[rows, :], wo_v[...], (((1,), (1,)), ((), ())), preferred_element_type=f32)
                dz_v[rows, :] = (dh * slope_v[rows, :]).astype(bf16)
                return c

            lax.fori_loop(0, ROWS // 256, tile, 0)
            by_phase(step + 1, wo_make, start)
            by_phase(step + 1, z_make, wait)

        @pl.when(live & ((part == 1) | (part == 2)))
        def _():
            own = step % N_SUM
            is_a = (part == 1) == (core == 1)
            slot_a = jnp.where(core == 0, own, N_SUM)
            slot_b = jnp.where(core == 0, N_SUM, own)

            @pl.when(is_a)
            def _():
                def grad_a(nb, c):
                    cols = pl.ds(pl.multiple_of(nb * 256, 256), 256)
                    gelu_rows(nb * 384, 384)
                    total = None
                    for m in range(2):
                        rows = pl.ds(m * MICRO, MICRO)
                        got = lax.dot_general(h_v[rows, :], dy_v[rows, cols], (((0,), (0,)), ((), ())), preferred_element_type=f32)
                        got = got.astype(bf16).astype(f32)
                        total = got if total is None else total + got
                    for q in range(4):
                        for j in range(2):
                            here = pl.ds(pl.multiple_of((2 * nb + j) * 128, 128), 128)
                            big[slot_a, q // 2, q % 2, here, :] = total[128 * q:128 * q + 128, 128 * j:128 * j + 128]
                    return c

                lax.fori_loop(0, 3, grad_a, 0)

            @pl.when(jnp.logical_not(is_a))
            def _():
                @pl.when(step == 0)
                def _():
                    load_2.wait()

                @pl.when(step == UNITS)
                def _():
                    load_1.wait()

                def grad_b(nb, c):
                    cols = pl.ds(pl.multiple_of(nb * 256, 256), 256)
                    gelu_rows(1152 + nb * 448, 448)
                    total = None
                    for m in range(2):
                        rows = pl.ds(m * MICRO, MICRO)
                        got = lax.dot_general(x_v[rows, :], dz_v[rows, cols], (((0,), (0,)), ((), ())), preferred_element_type=f32)
                        got = got.astype(bf16).astype(f32)
                        total = got if total is None else total + got
                    for q in range(4):
                        for j in range(2):
                            here = pl.ds(pl.multiple_of((2 * nb + j) * 192, 64), 192)
                            big[slot_b, q // 2, q % 2, here, :] = total[192 * q:192 * q + 192, 128 * j:128 * j + 128]
                    return c

                lax.fori_loop(0, 2, grad_b, 0)

                @pl.when(step == UNITS - 1)
                def _():
                    load_1.start()

            @pl.when(part == 1)
            def _():
                d2d_copy(step).start()

            @pl.when(part == 2)
            def _():
                by_phase(step + 2, z_make, start)

        @pl.when((step < UNITS) & (part == 3))
        def _():
            for cp in wi_copies(step):
                cp.wait()

            def back(t, c):
                rows = pl.ds(pl.multiple_of(t * 512, 512), 512)
                add = lax.dot_general(dz_v[rows, :], wi_v[...], (((1,), (1,)), ((), ())), preferred_element_type=f32)
                acc_v[rows, :] = jnp.where(step == 0, dy_v[rows, :].astype(f32), acc_v[rows, :]) + add
                return c

            lax.fori_loop(0, ROWS // 512, back, 0)

            @pl.when(step < UNITS - 1)
            def _():
                for cp in wi_copies(step + 1):
                    cp.start()

            @pl.when(step == UNITS - 1)
            def _():
                def close(t, c):
                    rows = pl.ds(pl.multiple_of(t * 32, 32), 32)
                    dy_v[rows, :] = acc_v[rows, :].astype(bf16)
                    return c

                lax.fori_loop(0, ROWS // 32, close, 0)

        early = (part == 3) & (step < UNITS)
        late = (part == 0) & (step > UNITS) & (step <= STEPS)

        @pl.when(early | late)
        def _():
            chip_sum(jnp.where(part == 3, step, step - 1))

        return run_ticks(tick, seen)

    lax.fori_loop(0, TICKS, body, (jnp.int32(0),) * (len(TAKES) + 1))


def solution(mesh):
    row_spec = P(('dz', 'dy', 'dx'), None)
    full_spec = P(None, None)

    def per_device(*arrays):
        f32, bf16 = jnp.float32, jnp.bfloat16
        landings = []
        for idx, stage in STAGES:
            ny, nz = landing_dims(ORDERS[idx], stage)
            landings.append(pltpu.VMEM((SLOTS, ny, nz, max(ROWS_ONE[idx], ROWS_TWO[idx]), 128), f32))
        out = pl.pallas_call(
            kernel,
            out_shape=jax.ShapeDtypeStruct((4608, 128), f32),
            in_specs=[pl.BlockSpec(memory_space=pl.ANY)] * 8,
            out_specs=pl.BlockSpec(memory_space=pltpu.VMEM),
            scratch_shapes=[
                pltpu.VMEM((ROWS, D), bf16),
                pltpu.VMEM((ROWS, D), bf16),
                pltpu.VMEM((ROWS, D), f32),
                pltpu.VMEM((ROWS, WIDE), bf16),
                pltpu.VMEM((ROWS, WIDE), bf16),
                pltpu.VMEM((ROWS, WIDE), bf16),
                pltpu.VMEM((ROWS, WIDE), f32),
                pltpu.VMEM((ROWS, WIDE), bf16),
                pltpu.VMEM((WIDE, D), bf16),
                pltpu.VMEM((D, WIDE), bf16),
                pltpu.VMEM((N_SUM + 1, 2, 2, 768, 128), f32),
                pltpu.VMEM((2, 2, 2, 768, 128), f32),
                *landings,
                pltpu.SemaphoreType.DMA((3,)),
                pltpu.SemaphoreType.DMA((4,)),
                pltpu.SemaphoreType.DMA((4,)),
                pltpu.SemaphoreType.DMA((4,)),
                pltpu.SemaphoreType.DMA((1,)),
                pltpu.SemaphoreType.DMA((2,)),
                pltpu.SemaphoreType.DMA((len(STAGES), SLOTS)),
                pltpu.SemaphoreType.DMA((len(STAGES), SLOTS)),
            ],
            compiler_params=pltpu.CompilerParams(collective_id=0, has_side_effects=True, vmem_limit_bytes=67043328),
        )(*arrays)
        return out.reshape(-1)

    return jax.shard_map(per_device, mesh=mesh, in_specs=(row_spec,) * 5 + (full_spec,) * 3, out_specs=P(('dx', 'dy', 'dz')), check_vma=False)
```

```python
import math

import jax
import jax.numpy as jnp
from jax import lax
from jax.experimental import pallas as pl
from jax.experimental.pallas import tpu as pltpu
from jax.sharding import PartitionSpec as P

MESH = pl.DeviceIdType.MESH
D = 768
FF = 3072
ROWS = 2048
MICRO = 1024
UNITS = 6
WIDE = 512
STEPS = 2 * UNITS
SLOTS = 6
TILE = 1024
ORDERS = ('yzx', 'zyx', 'xyz', 'xzy', 'wyzx', 'wzyx')
TAKES = {
    (0, 0): (7, 11, 15, 19, 23, 27, 37, 41, 45, 51, 58, 64),
    (0, 1): (13, 17, 21, 25, 29, 33, 45, 53, 60, 66, 69, 71),
    (0, 2): (17, 21, 27, 33, 37, 39, 48, 55, 61, 66, 69, 72),
    (1, 0): (7, 11, 15, 19, 23, 29, 33, 37, 41, 45, 51, 58),
    (1, 1): (13, 17, 21, 25, 29, 35, 41, 47, 54, 58, 64, 67),
    (1, 2): (15, 19, 23, 29, 35, 41, 54, 60, 66, 69, 71, 71),
    (2, 0): (9, 11, 15, 19, 23, 29),
    (2, 1): (13, 17, 21, 25, 29, 37),
    (2, 2): (17, 21, 25, 29, 37, 47),
    (2, 3): (21, 27, 33, 37, 41, 49),
}
FINISH = (21, 27, 33, 37, 41, 49, 54, 60, 66, 69, 71, 72)
N_SUM = 7
TICKS = 73
ROWS_ONE = (224, 224, 64, 64, 96, 96)
ROWS_TWO = (320, 320, 64, 64, 0, 0)
ROOT = math.sqrt(2.0 / math.pi)
CUBE = 0.044715


def gelu_pair(val):
    sq = val * val
    tan = jnp.tanh(val * (sq * (ROOT * CUBE) + ROOT))
    cdf = 0.5 * tan + 0.5
    bump = val * (cdf * (1.0 - cdf))
    return val * cdf, cdf + bump * (sq * (6.0 * ROOT * CUBE) + 2.0 * ROOT)


def landing_dims(order, stage):
    done = order[:stage + 1]
    return (1 if 'y' in done else 2), (1 if 'z' in done else 2)


def stage_list():
    return [(idx, stage) for idx, order in enumerate(ORDERS) for stage in range(len(order))]


STAGES = stage_list()


def kernel(a1_hbm, z1_hbm, a2_hbm, z2_hbm, g_hbm, wi_hbm, wo1_hbm, wo2_hbm, out_ref,
           dy_v, x_v, acc_v, z_v, hnew_v, h_v, slope_v, dz_v, wo_v, wi_v, big, drecv, *rest):
    landings = dict(zip(STAGES, rest[:len(STAGES)]))
    isem, zsem, osem, wsem, dsend_sem, drecv_sem, send_sem, recv_sem = rest[len(STAGES):]
    f32, bf16 = jnp.float32, jnp.bfloat16
    dx, y, z = lax.axis_index('dx'), lax.axis_index('dy'), lax.axis_index('dz')
    x, core = dx // 2, dx % 2
    peers = {'x': {'dx': (dx + 2) % 4}, 'y': {'dy': 1 - y}, 'z': {'dz': 1 - z}, 'c': {'dx': dx + 1 - 2 * core}}
    peers['w'] = peers['x']

    barrier = pltpu.get_barrier_semaphore()
    for name in 'xyzc':
        pl.semaphore_signal(barrier, inc=1, device_id=peers[name], device_id_type=MESH)

    load_g = pltpu.make_async_copy(g_hbm, dy_v, isem.at[0])
    load_2 = pltpu.make_async_copy(a2_hbm, x_v, isem.at[1])
    load_1 = pltpu.make_async_copy(a1_hbm, x_v, isem.at[2])

    def columns(unit, quarter):
        return pl.ds(pl.multiple_of(quarter * 768 + unit * 128, 128), 128), pl.ds(quarter * 128, 128)

    def z_copies(unit, hbm):
        pairs = [columns(unit, q) for q in range(4)]
        return [pltpu.make_async_copy(hbm.at[:, get], z_v.at[:, put], zsem.at[q]) for q, (get, put) in enumerate(pairs)]

    def wo_copies(unit, hbm):
        pairs = [columns(unit, q) for q in range(4)]
        return [pltpu.make_async_copy(hbm.at[get, :], wo_v.at[put, :], osem.at[q]) for q, (get, put) in enumerate(pairs)]

    def wi_copies(unit):
        pairs = [columns(unit, q) for q in range(4)]
        return [pltpu.make_async_copy(wi_hbm.at[:, get], wi_v.at[:, put], wsem.at[q]) for q, (get, put) in enumerate(pairs)]

    def by_phase(step, make, action):
        @pl.when(step < UNITS)
        def _():
            for cp in make(step, 0):
                action(cp)

        @pl.when((step >= UNITS) & (step < STEPS))
        def _():
            for cp in make(step - UNITS, 1):
                action(cp)

    def z_make(unit, phase):
        return z_copies(unit, z1_hbm if phase else z2_hbm)

    def wo_make(unit, phase):
        return wo_copies(unit, wo1_hbm if phase else wo2_hbm)

    def start(cp):
        cp.start()

    def wait(cp):
        cp.wait()

    for cp in z_copies(0, z2_hbm):
        cp.start()
    for cp in wo_copies(0, wo2_hbm):
        cp.start()
    load_g.start()
    load_2.start()
    for cp in wi_copies(0):
        cp.start()

    def gelu_rows(start, count):
        for k in range(count // 32):
            rows = pl.ds(pl.multiple_of(start + k * 32, 32), 32)
            hid, slope = gelu_pair(z_v[rows, :].astype(f32))
            hnew_v[rows, :] = hid.astype(bf16)
            slope_v[rows, :] = slope

    for cp in z_copies(0, z2_hbm):
        cp.wait()

    def first_gelu(t, c):
        gelu_rows(t * 128, 128)
        return c

    lax.fori_loop(0, ROWS // 128, first_gelu, 0)
    for cp in z_copies(1, z2_hbm):
        cp.start()
    load_g.wait()
    pl.semaphore_wait(barrier, 4)

    def d2d_copy(unit):
        return pltpu.make_async_remote_copy(src_ref=big.at[N_SUM], dst_ref=drecv.at[unit % 2], send_sem=dsend_sem.at[0],
                                            recv_sem=drecv_sem.at[unit % 2], device_id=peers['c'], device_id_type=MESH)

    def placed(phase):
        sizes = (ROWS_ONE, ROWS_TWO)[phase]
        starts = [sum(sizes[:k]) for k in range(len(sizes))]
        return list(zip(starts, sizes))

    def stage_copy(idx, stage, unit, phase):
        order = ORDERS[idx]
        first, rows = placed(phase)[idx]
        done, axis = order[:stage], order[stage]
        at_y = pl.ds(1 - y, 1) if axis == 'y' else pl.ds(y, 1) if 'y' in done else pl.ds(0, 2)
        at_z = pl.ds(1 - z, 1) if axis == 'z' else pl.ds(z, 1) if 'z' in done else pl.ds(0, 2)
        slot, sem = unit % SLOTS, STAGES.index((idx, stage))
        return pltpu.make_async_remote_copy(src_ref=big.at[unit % N_SUM, at_y, at_z, pl.ds(first, rows), :],
                                            dst_ref=landings[idx, stage].at[slot, :, :, pl.ds(0, rows), :],
                                            send_sem=send_sem.at[sem, slot], recv_sem=recv_sem.at[sem, slot],
                                            device_id=peers[axis], device_id_type=MESH)

    def roles(idx, stage, phase):
        order = ORDERS[idx]
        if order[stage] == 'w':
            return x == phase, x != phase
        if order[stage] == 'x':
            return x != phase, x == phase
        done = order[:stage]
        if 'x' in done:
            return x == phase, x == phase
        if 'w' in done:
            return x != phase, x != phase
        return None, None

    def guarded(cond, body):
        if cond is None:
            body()
        else:
            pl.when(cond)(body)

    def stage_send(idx, stage, unit, phase):
        guarded(roles(idx, stage, phase)[0], lambda: stage_copy(idx, stage, unit, phase).start())

    def stage_take(idx, stage, unit, phase):
        order = ORDERS[idx]
        first, rows = placed(phase)[idx]
        send_if, recv_if = roles(idx, stage, phase)
        ny, nz = landing_dims(order, stage)
        land, done = landings[idx, stage], order[:stage + 1]
        back = order[0] == 'w' and order[stage] == 'x'
        size = max(n for n in (128, 112, 96, 80, 64, 48, 32) if rows % n == 0)

        def take():
            stage_copy(idx, stage, unit, phase).wait_recv()
            for iy in range(ny):
                for iz in range(nz):
                    at_y = y if 'y' in done else iy
                    at_z = z if 'z' in done else iz

                    def chunk(k, carry):
                        offset = pl.multiple_of(k * size, 16)
                        here = (unit % N_SUM, at_y, at_z, pl.ds(first + offset, size), slice(None))
                        got = land[unit % SLOTS, iy, iz, pl.ds(offset, size), :]
                        big[here] = got if back else big[here] + got
                        return carry

                    lax.fori_loop(0, rows // size, chunk, 0)

        guarded(send_if, lambda: stage_copy(idx, stage, unit, phase).wait_send())
        guarded(recv_if, take)

    def part_list(phase):
        return [idx for idx in range(len(ORDERS)) if placed(phase)[idx][1]]

    def chip_sum(unit):
        d2d_copy(unit).wait()
        for iy in range(2):
            for iz in range(2):
                def chunk(k, carry):
                    here = pl.ds(pl.multiple_of(k * 128, 128), 128)
                    big[unit % N_SUM, iy, iz, here, :] = big[unit % N_SUM, iy, iz, here, :] + drecv[unit % 2, iy, iz, here, :]
                    return carry

                lax.fori_loop(0, 768 // 128, chunk, 0)
        for phase in range(2):
            @pl.when(unit // UNITS == phase)
            def _(phase=phase):
                for idx in part_list(phase):
                    stage_send(idx, 0, unit, phase)

    def finish(unit):
        sum_slot, pos = unit % N_SUM, unit % UNITS

        @pl.when((x == unit // UNITS) & (core == 0))
        def _():
            for j in range(6):
                out_ref[pl.ds(768 * pos + j, 128, stride=6), :] = big[sum_slot, y, z, pl.ds(128 * j, 128), :]

        @pl.when((x == unit // UNITS) & (core == 1))
        def _():
            for q in range(4):
                out_ref[pl.ds(6 * q + pos, 192, stride=24), :] = big[sum_slot, y, z, pl.ds(192 * q, 192), :]

    def reached(tick, row):
        total = jnp.int32(0)
        for value in row:
            total = total + jnp.where(tick >= value, 1, 0)
        return total

    def run_ticks(tick, seen):
        now = []
        for place, (key, row) in enumerate(sorted(TAKES.items())):
            group, stage = key
            count = reached(tick, row)

            def one(unit, carry):
                for phase in range(2):
                    members = [i for i in (2 * group, 2 * group + 1) if placed(phase)[i][1]]
                    if not members:
                        continue

                    @pl.when(unit // UNITS == phase)
                    def _(phase=phase, members=members):
                        for idx in members:
                            stage_take(idx, stage, unit, phase)
                            if stage + 1 < len(ORDERS[idx]):
                                stage_send(idx, stage + 1, unit, phase)
                return carry

            lax.fori_loop(seen[place], count, one, 0)
            now.append(count)
        count = reached(tick, FINISH)

        def last(unit, carry):
            finish(unit)
            return carry

        lax.fori_loop(seen[-1], count, last, 0)
        now.append(count)
        return tuple(now)

    def body(tick, seen):
        step, part = tick // 4, tick % 4
        live = step < STEPS

        @pl.when(live & (part == 0))
        def _():
            by_phase(step, wo_make, wait)

            def tile(t, c):
                rows = pl.ds(pl.multiple_of(t * TILE, TILE), TILE)
                h_v[rows, :] = hnew_v[rows, :]
                dh = lax.dot_general(dy_v[rows, :], wo_v[...], (((1,), (1,)), ((), ())), preferred_element_type=f32)
                dz_v[rows, :] = (dh * slope_v[rows, :]).astype(bf16)
                return c

            lax.fori_loop(0, ROWS // TILE, tile, 0)
            by_phase(step + 1, wo_make, start)
            by_phase(step + 1, z_make, wait)

        @pl.when(live & ((part == 1) | (part == 2)))
        def _():
            own = step % N_SUM
            is_a = (part == 1) == (core == 1)
            slot_a = jnp.where(core == 0, own, N_SUM)
            slot_b = jnp.where(core == 0, N_SUM, own)

            @pl.when(is_a)
            def _():
                def grad_a(nb, c):
                    cols = pl.ds(pl.multiple_of(nb * 256, 256), 256)
                    gelu_rows(nb * 384, 384)
                    total = None
                    for m in range(2):
                        rows = pl.ds(m * MICRO, MICRO)
                        got = lax.dot_general(h_v[rows, :], dy_v[rows, cols], (((0,), (0,)), ((), ())), preferred_element_type=f32)
                        got = got.astype(bf16).astype(f32)
                        total = got if total is None else total + got
                    for q in range(4):
                        for j in range(2):
                            here = pl.ds(pl.multiple_of((2 * nb + j) * 128, 128), 128)
                            big[slot_a, q // 2, q % 2, here, :] = total[128 * q:128 * q + 128, 128 * j:128 * j + 128]
                    return c

                lax.fori_loop(0, 3, grad_a, 0)

            @pl.when(jnp.logical_not(is_a))
            def _():
                @pl.when(step == 0)
                def _():
                    load_2.wait()

                @pl.when(step == UNITS)
                def _():
                    load_1.wait()

                def grad_b(nb, c):
                    cols = pl.ds(pl.multiple_of(nb * 256, 256), 256)
                    gelu_rows(1152 + nb * 448, 448)
                    total = None
                    for m in range(2):
                        rows = pl.ds(m * MICRO, MICRO)
                        got = lax.dot_general(x_v[rows, :], dz_v[rows, cols], (((0,), (0,)), ((), ())), preferred_element_type=f32)
                        got = got.astype(bf16).astype(f32)
                        total = got if total is None else total + got
                    for q in range(4):
                        for j in range(2):
                            here = pl.ds(pl.multiple_of((2 * nb + j) * 192, 64), 192)
                            big[slot_b, q // 2, q % 2, here, :] = total[192 * q:192 * q + 192, 128 * j:128 * j + 128]
                    return c

                lax.fori_loop(0, 2, grad_b, 0)

                @pl.when(step == UNITS - 1)
                def _():
                    load_1.start()

            @pl.when(part == 1)
            def _():
                d2d_copy(step).start()

            @pl.when(part == 2)
            def _():
                by_phase(step + 2, z_make, start)

        @pl.when((step < UNITS) & (part == 3))
        def _():
            for cp in wi_copies(step):
                cp.wait()

            def back(t, c):
                rows = pl.ds(pl.multiple_of(t * TILE, TILE), TILE)
                add = lax.dot_general(dz_v[rows, :], wi_v[...], (((1,), (1,)), ((), ())), preferred_element_type=f32)
                acc_v[rows, :] = jnp.where(step == 0, dy_v[rows, :].astype(f32), acc_v[rows, :]) + add
                return c

            lax.fori_loop(0, ROWS // TILE, back, 0)

            @pl.when(step < UNITS - 1)
            def _():
                for cp in wi_copies(step + 1):
                    cp.start()

            @pl.when(step == UNITS - 1)
            def _():
                def close(t, c):
                    rows = pl.ds(pl.multiple_of(t * 32, 32), 32)
                    dy_v[rows, :] = acc_v[rows, :].astype(bf16)
                    return c

                lax.fori_loop(0, ROWS // 32, close, 0)

        early = (part == 3) & (step < UNITS)
        late = (part == 0) & (step > UNITS) & (step <= STEPS)

        @pl.when(early | late)
        def _():
            chip_sum(jnp.where(part == 3, step, step - 1))

        return run_ticks(tick, seen)

    lax.fori_loop(0, TICKS, body, (jnp.int32(0),) * (len(TAKES) + 1))


def solution(mesh):
    row_spec = P(('dz', 'dy', 'dx'), None)
    full_spec = P(None, None)

    def per_device(*arrays):
        f32, bf16 = jnp.float32, jnp.bfloat16
        landings = []
        for idx, stage in STAGES:
            ny, nz = landing_dims(ORDERS[idx], stage)
            landings.append(pltpu.VMEM((SLOTS, ny, nz, max(ROWS_ONE[idx], ROWS_TWO[idx]), 128), f32))
        out = pl.pallas_call(
            kernel,
            out_shape=jax.ShapeDtypeStruct((4608, 128), f32),
            in_specs=[pl.BlockSpec(memory_space=pl.ANY)] * 8,
            out_specs=pl.BlockSpec(memory_space=pltpu.VMEM),
            scratch_shapes=[
                pltpu.VMEM((ROWS, D), bf16),
                pltpu.VMEM((ROWS, D), bf16),
                pltpu.VMEM((ROWS, D), f32),
                pltpu.VMEM((ROWS, WIDE), bf16),
                pltpu.VMEM((ROWS, WIDE), bf16),
                pltpu.VMEM((ROWS, WIDE), bf16),
                pltpu.VMEM((ROWS, WIDE), f32),
                pltpu.VMEM((ROWS, WIDE), bf16),
                pltpu.VMEM((WIDE, D), bf16),
                pltpu.VMEM((D, WIDE), bf16),
                pltpu.VMEM((N_SUM + 1, 2, 2, 768, 128), f32),
                pltpu.VMEM((2, 2, 2, 768, 128), f32),
                *landings,
                pltpu.SemaphoreType.DMA((3,)),
                pltpu.SemaphoreType.DMA((4,)),
                pltpu.SemaphoreType.DMA((4,)),
                pltpu.SemaphoreType.DMA((4,)),
                pltpu.SemaphoreType.DMA((1,)),
                pltpu.SemaphoreType.DMA((2,)),
                pltpu.SemaphoreType.DMA((len(STAGES), SLOTS)),
                pltpu.SemaphoreType.DMA((len(STAGES), SLOTS)),
            ],
            compiler_params=pltpu.CompilerParams(collective_id=0, has_side_effects=True, vmem_limit_bytes=67043328),
        )(*arrays)
        return out.reshape(-1)

    return jax.shard_map(per_device, mesh=mesh, in_specs=(row_spec,) * 5 + (full_spec,) * 3, out_specs=P(('dx', 'dy', 'dz')), check_vma=False)
```

```python
import math

import jax
import jax.numpy as jnp
from jax import lax
from jax.experimental import pallas as pl
from jax.experimental.pallas import tpu as pltpu
from jax.sharding import PartitionSpec as P

MESH = pl.DeviceIdType.MESH
D = 768
FF = 3072
ROWS = 2048
MICRO = 1024
UNITS = 6
WIDE = 512
STEPS = 2 * UNITS
SLOTS = 6
TILE = 1024
ORDERS = ('yzx', 'zyx', 'xyz', 'xzy', 'wyzx', 'wzyx')
TAKES = {
    (0, 0): (5515944, 66568),
    (0, 1): (4281664, 9703456),
    (0, 2): (861440, 18096258),
    (1, 0): (5589672, 1032),
    (1, 1): (9590080, 2360352),
    (1, 2): (1198848, 27529248),
    (2, 0): (21840, 0),
    (2, 1): (283968, 0),
    (2, 2): (8672512, 0),
    (2, 3): (1385472, 4),
}
FINISH = (1385472, 27529252)
N_SUM = 7
TICKS = 73
ROWS_ONE = (224, 224, 64, 64, 96, 96)
ROWS_TWO = (320, 320, 64, 64, 0, 0)
ROOT = math.sqrt(2.0 / math.pi)
CUBE = 0.044715


def gelu_pair(val):
    sq = val * val
    tan = jnp.tanh(val * (sq * (ROOT * CUBE) + ROOT))
    cdf = 0.5 * tan + 0.5
    bump = val * (cdf * (1.0 - cdf))
    return val * cdf, cdf + bump * (sq * (6.0 * ROOT * CUBE) + 2.0 * ROOT)


def landing_dims(order, stage):
    done = order[:stage + 1]
    return (1 if 'y' in done else 2), (1 if 'z' in done else 2)


def stage_list():
    return [(idx, stage) for idx, order in enumerate(ORDERS) for stage in range(len(order))]


STAGES = stage_list()


def kernel(a1_hbm, z1_hbm, a2_hbm, z2_hbm, g_hbm, wi_hbm, wo1_hbm, wo2_hbm, out_ref,
           dy_v, x_v, acc_v, z_v, hnew_v, h_v, slope_v, dz_v, wo_v, wi_v, big, drecv, *rest):
    landings = dict(zip(STAGES, rest[:len(STAGES)]))
    isem, zsem, osem, wsem, dsend_sem, drecv_sem, send_sem, recv_sem = rest[len(STAGES):]
    f32, bf16 = jnp.float32, jnp.bfloat16
    dx, y, z = lax.axis_index('dx'), lax.axis_index('dy'), lax.axis_index('dz')
    x, core = dx // 2, dx % 2
    peers = {'x': {'dx': (dx + 2) % 4}, 'y': {'dy': 1 - y}, 'z': {'dz': 1 - z}, 'c': {'dx': dx + 1 - 2 * core}}
    peers['w'] = peers['x']

    barrier = pltpu.get_barrier_semaphore()
    for name in 'xyzc':
        pl.semaphore_signal(barrier, inc=1, device_id=peers[name], device_id_type=MESH)

    load_g = pltpu.make_async_copy(g_hbm, dy_v, isem.at[0])
    load_2 = pltpu.make_async_copy(a2_hbm, x_v, isem.at[1])
    load_1 = pltpu.make_async_copy(a1_hbm, x_v, isem.at[2])

    def columns(unit, quarter):
        return pl.ds(pl.multiple_of(quarter * 768 + unit * 128, 128), 128), pl.ds(quarter * 128, 128)

    def z_copies(unit, hbm):
        pairs = [columns(unit, q) for q in range(4)]
        return [pltpu.make_async_copy(hbm.at[:, get], z_v.at[:, put], zsem.at[q]) for q, (get, put) in enumerate(pairs)]

    def wo_copies(unit, hbm):
        pairs = [columns(unit, q) for q in range(4)]
        return [pltpu.make_async_copy(hbm.at[get, :], wo_v.at[put, :], osem.at[q]) for q, (get, put) in enumerate(pairs)]

    def wi_copies(unit):
        pairs = [columns(unit, q) for q in range(4)]
        return [pltpu.make_async_copy(wi_hbm.at[:, get], wi_v.at[:, put], wsem.at[q]) for q, (get, put) in enumerate(pairs)]

    def by_phase(step, make, action):
        @pl.when(step < UNITS)
        def _():
            for cp in make(step, 0):
                action(cp)

        @pl.when((step >= UNITS) & (step < STEPS))
        def _():
            for cp in make(step - UNITS, 1):
                action(cp)

    def z_make(unit, phase):
        return z_copies(unit, z1_hbm if phase else z2_hbm)

    def wo_make(unit, phase):
        return wo_copies(unit, wo1_hbm if phase else wo2_hbm)

    def start(cp):
        cp.start()

    def wait(cp):
        cp.wait()

    for cp in z_copies(0, z2_hbm):
        cp.start()
    for cp in wo_copies(0, wo2_hbm):
        cp.start()
    load_g.start()
    load_2.start()
    for cp in wi_copies(0):
        cp.start()

    def gelu_rows(start, count):
        for k in range(count // 32):
            rows = pl.ds(pl.multiple_of(start + k * 32, 32), 32)
            hid, slope = gelu_pair(z_v[rows, :].astype(f32))
            hnew_v[rows, :] = hid.astype(bf16)
            slope_v[rows, :] = slope

    for cp in z_copies(0, z2_hbm):
        cp.wait()

    def first_gelu(t, c):
        gelu_rows(t * 128, 128)
        return c

    lax.fori_loop(0, ROWS // 128, first_gelu, 0)
    for cp in z_copies(1, z2_hbm):
        cp.start()
    load_g.wait()
    pl.semaphore_wait(barrier, 4)

    def d2d_copy(unit):
        return pltpu.make_async_remote_copy(src_ref=big.at[N_SUM], dst_ref=drecv.at[unit % 2], send_sem=dsend_sem.at[0],
                                            recv_sem=drecv_sem.at[unit % 2], device_id=peers['c'], device_id_type=MESH)

    def placed(phase):
        sizes = (ROWS_ONE, ROWS_TWO)[phase]
        starts = [sum(sizes[:k]) for k in range(len(sizes))]
        return list(zip(starts, sizes))

    def stage_copy(idx, stage, unit, phase):
        order = ORDERS[idx]
        first, rows = placed(phase)[idx]
        done, axis = order[:stage], order[stage]
        at_y = pl.ds(1 - y, 1) if axis == 'y' else pl.ds(y, 1) if 'y' in done else pl.ds(0, 2)
        at_z = pl.ds(1 - z, 1) if axis == 'z' else pl.ds(z, 1) if 'z' in done else pl.ds(0, 2)
        slot, sem = unit % SLOTS, STAGES.index((idx, stage))
        return pltpu.make_async_remote_copy(src_ref=big.at[unit % N_SUM, at_y, at_z, pl.ds(first, rows), :],
                                            dst_ref=landings[idx, stage].at[slot, :, :, pl.ds(0, rows), :],
                                            send_sem=send_sem.at[sem, slot], recv_sem=recv_sem.at[sem, slot],
                                            device_id=peers[axis], device_id_type=MESH)

    def roles(idx, stage, phase):
        order = ORDERS[idx]
        if order[stage] == 'w':
            return x == phase, x != phase
        if order[stage] == 'x':
            return x != phase, x == phase
        done = order[:stage]
        if 'x' in done:
            return x == phase, x == phase
        if 'w' in done:
            return x != phase, x != phase
        return None, None

    def guarded(cond, body):
        if cond is None:
            body()
        else:
            pl.when(cond)(body)

    def stage_send(idx, stage, unit, phase):
        guarded(roles(idx, stage, phase)[0], lambda: stage_copy(idx, stage, unit, phase).start())

    def stage_take(idx, stage, unit, phase):
        order = ORDERS[idx]
        first, rows = placed(phase)[idx]
        send_if, recv_if = roles(idx, stage, phase)
        ny, nz = landing_dims(order, stage)
        land, done = landings[idx, stage], order[:stage + 1]
        back = order[0] == 'w' and order[stage] == 'x'
        size = max(n for n in (128, 112, 96, 80, 64, 48, 32) if rows % n == 0)

        def take():
            stage_copy(idx, stage, unit, phase).wait_recv()
            for iy in range(ny):
                for iz in range(nz):
                    at_y = y if 'y' in done else iy
                    at_z = z if 'z' in done else iz

                    def chunk(k, carry):
                        offset = pl.multiple_of(k * size, 16)
                        here = (unit % N_SUM, at_y, at_z, pl.ds(first + offset, size), slice(None))
                        got = land[unit % SLOTS, iy, iz, pl.ds(offset, size), :]
                        big[here] = got if back else big[here] + got
                        return carry

                    lax.fori_loop(0, rows // size, chunk, 0)

        guarded(send_if, lambda: stage_copy(idx, stage, unit, phase).wait_send())
        guarded(recv_if, take)

    def part_list(phase):
        return [idx for idx in range(len(ORDERS)) if placed(phase)[idx][1]]

    def chip_sum(unit):
        d2d_copy(unit).wait()
        for iy in range(2):
            for iz in range(2):
                def chunk(k, carry):
                    here = pl.ds(pl.multiple_of(k * 128, 128), 128)
                    big[unit % N_SUM, iy, iz, here, :] = big[unit % N_SUM, iy, iz, here, :] + drecv[unit % 2, iy, iz, here, :]
                    return carry

                lax.fori_loop(0, 768 // 128, chunk, 0)
        for phase in range(2):
            @pl.when(unit // UNITS == phase)
            def _(phase=phase):
                for idx in part_list(phase):
                    stage_send(idx, 0, unit, phase)

    def finish(unit):
        sum_slot, pos = unit % N_SUM, unit % UNITS

        @pl.when((x == unit // UNITS) & (core == 0))
        def _():
            for j in range(6):
                out_ref[pl.ds(768 * pos + j, 128, stride=6), :] = big[sum_slot, y, z, pl.ds(128 * j, 128), :]

        @pl.when((x == unit // UNITS) & (core == 1))
        def _():
            for q in range(4):
                out_ref[pl.ds(6 * q + pos, 192, stride=24), :] = big[sum_slot, y, z, pl.ds(192 * q, 192), :]

    def due(tick, words):
        word = jnp.where(tick < 4 * STEPS, words[0], words[1])
        place = jnp.where(tick < 4 * STEPS, tick // 2, tick - 4 * STEPS)
        return (word >> place) & 1

    def run_ticks(tick, seen):
        now = []
        for place, (key, words) in enumerate(sorted(TAKES.items())):
            group, stage = key
            unit, bit = seen[place], due(tick, words)
            for phase in range(2):
                members = [i for i in (2 * group, 2 * group + 1) if placed(phase)[i][1]]
                if not members:
                    continue

                @pl.when((bit == 1) & (unit // UNITS == phase))
                def _(phase=phase, members=members, unit=unit, stage=stage):
                    for idx in members:
                        stage_take(idx, stage, unit, phase)
                        if stage + 1 < len(ORDERS[idx]):
                            stage_send(idx, stage + 1, unit, phase)
            now.append(unit + bit)
        unit, bit = seen[-1], due(tick, FINISH)

        @pl.when(bit == 1)
        def _():
            finish(unit)
        now.append(unit + bit)
        return tuple(now)

    def body(tick, seen):
        step, part = tick // 4, tick % 4
        live = step < STEPS

        @pl.when(live & (part == 0))
        def _():
            by_phase(step, wo_make, wait)

            def tile(t, c):
                rows = pl.ds(pl.multiple_of(t * TILE, TILE), TILE)
                h_v[rows, :] = hnew_v[rows, :]
                dh = lax.dot_general(dy_v[rows, :], wo_v[...], (((1,), (1,)), ((), ())), preferred_element_type=f32)
                dz_v[rows, :] = (dh * slope_v[rows, :]).astype(bf16)
                return c

            lax.fori_loop(0, ROWS // TILE, tile, 0)
            by_phase(step + 1, wo_make, start)
            by_phase(step + 1, z_make, wait)

        @pl.when(live & ((part == 1) | (part == 2)))
        def _():
            own = step % N_SUM
            is_a = (part == 1) == (core == 1)
            slot_a = jnp.where(core == 0, own, N_SUM)
            slot_b = jnp.where(core == 0, N_SUM, own)

            @pl.when(is_a)
            def _():
                def grad_a(nb, c):
                    cols = pl.ds(pl.multiple_of(nb * 256, 256), 256)
                    gelu_rows(nb * 384, 384)
                    total = None
                    for m in range(2):
                        rows = pl.ds(m * MICRO, MICRO)
                        got = lax.dot_general(h_v[rows, :], dy_v[rows, cols], (((0,), (0,)), ((), ())), preferred_element_type=f32)
                        got = got.astype(bf16).astype(f32)
                        total = got if total is None else total + got
                    for q in range(4):
                        for j in range(2):
                            here = pl.ds(pl.multiple_of((2 * nb + j) * 128, 128), 128)
                            big[slot_a, q // 2, q % 2, here, :] = total[128 * q:128 * q + 128, 128 * j:128 * j + 128]
                    return c

                lax.fori_loop(0, 3, grad_a, 0)

            @pl.when(jnp.logical_not(is_a))
            def _():
                @pl.when(step == 0)
                def _():
                    load_2.wait()

                @pl.when(step == UNITS)
                def _():
                    load_1.wait()

                def grad_b(nb, c):
                    cols = pl.ds(pl.multiple_of(nb * 256, 256), 256)
                    gelu_rows(1152 + nb * 448, 448)
                    total = None
                    for m in range(2):
                        rows = pl.ds(m * MICRO, MICRO)
                        got = lax.dot_general(x_v[rows, :], dz_v[rows, cols], (((0,), (0,)), ((), ())), preferred_element_type=f32)
                        got = got.astype(bf16).astype(f32)
                        total = got if total is None else total + got
                    for q in range(4):
                        for j in range(2):
                            here = pl.ds(pl.multiple_of((2 * nb + j) * 192, 64), 192)
                            big[slot_b, q // 2, q % 2, here, :] = total[192 * q:192 * q + 192, 128 * j:128 * j + 128]
                    return c

                lax.fori_loop(0, 2, grad_b, 0)

                @pl.when(step == UNITS - 1)
                def _():
                    load_1.start()

            @pl.when(part == 1)
            def _():
                d2d_copy(step).start()

            @pl.when(part == 2)
            def _():
                by_phase(step + 2, z_make, start)

        @pl.when((step < UNITS) & (part == 3))
        def _():
            for cp in wi_copies(step):
                cp.wait()

            def back(t, c):
                rows = pl.ds(pl.multiple_of(t * TILE, TILE), TILE)
                add = lax.dot_general(dz_v[rows, :], wi_v[...], (((1,), (1,)), ((), ())), preferred_element_type=f32)
                acc_v[rows, :] = jnp.where(step == 0, dy_v[rows, :].astype(f32), acc_v[rows, :]) + add
                return c

            lax.fori_loop(0, ROWS // TILE, back, 0)

            @pl.when(step < UNITS - 1)
            def _():
                for cp in wi_copies(step + 1):
                    cp.start()

            @pl.when(step == UNITS - 1)
            def _():
                def close(t, c):
                    rows = pl.ds(pl.multiple_of(t * 32, 32), 32)
                    dy_v[rows, :] = acc_v[rows, :].astype(bf16)
                    return c

                lax.fori_loop(0, ROWS // 32, close, 0)

        early = (part == 3) & (step < UNITS)
        late = (part == 0) & (step > UNITS) & (step <= STEPS)

        @pl.when(early | late)
        def _():
            chip_sum(jnp.where(part == 3, step, step - 1))

        return lax.cond((tick % 2 == 1) | (tick >= 4 * STEPS), lambda kept: run_ticks(tick, kept), lambda kept: kept, seen)

    lax.fori_loop(0, TICKS, body, (jnp.int32(0),) * (len(TAKES) + 1))


def solution(mesh):
    row_spec = P(('dz', 'dy', 'dx'), None)
    full_spec = P(None, None)

    def per_device(*arrays):
        f32, bf16 = jnp.float32, jnp.bfloat16
        landings = []
        for idx, stage in STAGES:
            ny, nz = landing_dims(ORDERS[idx], stage)
            landings.append(pltpu.VMEM((SLOTS, ny, nz, max(ROWS_ONE[idx], ROWS_TWO[idx]), 128), f32))
        out = pl.pallas_call(
            kernel,
            out_shape=jax.ShapeDtypeStruct((4608, 128), f32),
            in_specs=[pl.BlockSpec(memory_space=pl.ANY)] * 8,
            out_specs=pl.BlockSpec(memory_space=pltpu.VMEM),
            scratch_shapes=[
                pltpu.VMEM((ROWS, D), bf16),
                pltpu.VMEM((ROWS, D), bf16),
                pltpu.VMEM((ROWS, D), f32),
                pltpu.VMEM((ROWS, WIDE), bf16),
                pltpu.VMEM((ROWS, WIDE), bf16),
                pltpu.VMEM((ROWS, WIDE), bf16),
                pltpu.VMEM((ROWS, WIDE), f32),
                pltpu.VMEM((ROWS, WIDE), bf16),
                pltpu.VMEM((WIDE, D), bf16),
                pltpu.VMEM((D, WIDE), bf16),
                pltpu.VMEM((N_SUM + 1, 2, 2, 768, 128), f32),
                pltpu.VMEM((2, 2, 2, 768, 128), f32),
                *landings,
                pltpu.SemaphoreType.DMA((3,)),
                pltpu.SemaphoreType.DMA((4,)),
                pltpu.SemaphoreType.DMA((4,)),
                pltpu.SemaphoreType.DMA((4,)),
                pltpu.SemaphoreType.DMA((1,)),
                pltpu.SemaphoreType.DMA((2,)),
                pltpu.SemaphoreType.DMA((len(STAGES), SLOTS)),
                pltpu.SemaphoreType.DMA((len(STAGES), SLOTS)),
            ],
            compiler_params=pltpu.CompilerParams(collective_id=0, has_side_effects=True, vmem_limit_bytes=67043328),
        )(*arrays)
        return out.reshape(-1)

    return jax.shard_map(per_device, mesh=mesh, in_specs=(row_spec,) * 5 + (full_spec,) * 3, out_specs=P(('dx', 'dy', 'dz')), check_vma=False)
```

```python
import math

import jax
import jax.numpy as jnp
from jax import lax
from jax.experimental import pallas as pl
from jax.experimental.pallas import tpu as pltpu
from jax.sharding import PartitionSpec as P

MESH = pl.DeviceIdType.MESH
D = 768
FF = 3072
ROWS = 2048
MICRO = 1024
UNITS = 6
WIDE = 512
STEPS = 2 * UNITS
SLOTS = 6
TILE = 1024
ORDERS = ('yzx', 'zyx', 'xyz', 'xzy', 'wyzx', 'wzyx')
TAKES = {
    (0, 0): (5393064, 2114),
    (0, 1): (1348928, 86152),
    (0, 2): (300288, 299278),
    (1, 0): (5589672, 68),
    (1, 1): (5327520, 41218),
    (1, 2): (608896, 233736),
    (2, 0): (9590096, 8736),
    (2, 1): (824640, 86082),
    (2, 2): (12883200, 463360),
    (2, 3): (594944, 7379970),
}
FINISH = (594944, 7379970)
N_SUM = 8
TICKS = 71
ROWS_ONE = (224, 224, 48, 48, 112, 112)
ROWS_TWO = (256, 256, 48, 48, 80, 80)
ROOT = math.sqrt(2.0 / math.pi)
CUBE = 0.044715


def gelu_pair(val):
    sq = val * val
    tan = jnp.tanh(val * (sq * (ROOT * CUBE) + ROOT))
    cdf = 0.5 * tan + 0.5
    bump = val * (cdf * (1.0 - cdf))
    return val * cdf, cdf + bump * (sq * (6.0 * ROOT * CUBE) + 2.0 * ROOT)


def landing_dims(order, stage):
    done = order[:stage + 1]
    return (1 if 'y' in done else 2), (1 if 'z' in done else 2)


def stage_list():
    return [(idx, stage) for idx, order in enumerate(ORDERS) for stage in range(len(order))]


STAGES = stage_list()


def kernel(a1_hbm, z1_hbm, a2_hbm, z2_hbm, g_hbm, wi_hbm, wo1_hbm, wo2_hbm, out_ref,
           dy_v, x_v, acc_v, z_v, hnew_v, h_v, slope_v, dz_v, wo_v, wi_v, big, drecv, *rest):
    landings = dict(zip(STAGES, rest[:len(STAGES)]))
    isem, zsem, osem, wsem, dsend_sem, drecv_sem, send_sem, recv_sem = rest[len(STAGES):]
    f32, bf16 = jnp.float32, jnp.bfloat16
    dx, y, z = lax.axis_index('dx'), lax.axis_index('dy'), lax.axis_index('dz')
    x, core = dx // 2, dx % 2
    peers = {'x': {'dx': (dx + 2) % 4}, 'y': {'dy': 1 - y}, 'z': {'dz': 1 - z}, 'c': {'dx': dx + 1 - 2 * core}}
    peers['w'] = peers['x']

    barrier = pltpu.get_barrier_semaphore()
    for name in 'xyzc':
        pl.semaphore_signal(barrier, inc=1, device_id=peers[name], device_id_type=MESH)

    load_g = pltpu.make_async_copy(g_hbm, dy_v, isem.at[0])
    load_2 = pltpu.make_async_copy(a2_hbm, x_v, isem.at[1])
    load_1 = pltpu.make_async_copy(a1_hbm, x_v, isem.at[2])

    def columns(unit, quarter):
        return pl.ds(pl.multiple_of(quarter * 768 + unit * 128, 128), 128), pl.ds(quarter * 128, 128)

    def z_copies(unit, hbm):
        pairs = [columns(unit, q) for q in range(4)]
        return [pltpu.make_async_copy(hbm.at[:, get], z_v.at[:, put], zsem.at[q]) for q, (get, put) in enumerate(pairs)]

    def wo_copies(unit, hbm):
        pairs = [columns(unit, q) for q in range(4)]
        return [pltpu.make_async_copy(hbm.at[get, :], wo_v.at[put, :], osem.at[q]) for q, (get, put) in enumerate(pairs)]

    def wi_copies(unit):
        pairs = [columns(unit, q) for q in range(4)]
        return [pltpu.make_async_copy(wi_hbm.at[:, get], wi_v.at[:, put], wsem.at[q]) for q, (get, put) in enumerate(pairs)]

    def by_phase(step, make, action):
        @pl.when(step < UNITS)
        def _():
            for cp in make(step, 0):
                action(cp)

        @pl.when((step >= UNITS) & (step < STEPS))
        def _():
            for cp in make(step - UNITS, 1):
                action(cp)

    def z_make(unit, phase):
        return z_copies(unit, z1_hbm if phase else z2_hbm)

    def wo_make(unit, phase):
        return wo_copies(unit, wo1_hbm if phase else wo2_hbm)

    def start(cp):
        cp.start()

    def wait(cp):
        cp.wait()

    for cp in z_copies(0, z2_hbm):
        cp.start()
    for cp in wo_copies(0, wo2_hbm):
        cp.start()
    load_g.start()
    load_2.start()
    for cp in wi_copies(0):
        cp.start()

    def gelu_rows(start, count):
        for k in range(count // 32):
            rows = pl.ds(pl.multiple_of(start + k * 32, 32), 32)
            hid, slope = gelu_pair(z_v[rows, :].astype(f32))
            hnew_v[rows, :] = hid.astype(bf16)
            slope_v[rows, :] = slope

    for cp in z_copies(0, z2_hbm):
        cp.wait()

    def first_gelu(t, c):
        gelu_rows(t * 128, 128)
        return c

    lax.fori_loop(0, ROWS // 128, first_gelu, 0)
    for cp in z_copies(1, z2_hbm):
        cp.start()
    load_g.wait()
    pl.semaphore_wait(barrier, 4)

    def d2d_copy(unit):
        return pltpu.make_async_remote_copy(src_ref=big.at[N_SUM], dst_ref=drecv.at[unit % 2], send_sem=dsend_sem.at[0],
                                            recv_sem=drecv_sem.at[unit % 2], device_id=peers['c'], device_id_type=MESH)

    def placed(phase):
        sizes = (ROWS_ONE, ROWS_TWO)[phase]
        starts = [sum(sizes[:k]) for k in range(len(sizes))]
        return list(zip(starts, sizes))

    def stage_copy(idx, stage, unit, phase):
        order = ORDERS[idx]
        first, rows = placed(phase)[idx]
        done, axis = order[:stage], order[stage]
        at_y = pl.ds(1 - y, 1) if axis == 'y' else pl.ds(y, 1) if 'y' in done else pl.ds(0, 2)
        at_z = pl.ds(1 - z, 1) if axis == 'z' else pl.ds(z, 1) if 'z' in done else pl.ds(0, 2)
        slot, sem = unit % SLOTS, STAGES.index((idx, stage))
        return pltpu.make_async_remote_copy(src_ref=big.at[unit % N_SUM, at_y, at_z, pl.ds(first, rows), :],
                                            dst_ref=landings[idx, stage].at[slot, :, :, pl.ds(0, rows), :],
                                            send_sem=send_sem.at[sem, slot], recv_sem=recv_sem.at[sem, slot],
                                            device_id=peers[axis], device_id_type=MESH)

    def roles(idx, stage, phase):
        order = ORDERS[idx]
        if order[stage] == 'w':
            return x == phase, x != phase
        if order[stage] == 'x':
            return x != phase, x == phase
        done = order[:stage]
        if 'x' in done:
            return x == phase, x == phase
        if 'w' in done:
            return x != phase, x != phase
        return None, None

    def guarded(cond, body):
        if cond is None:
            body()
        else:
            pl.when(cond)(body)

    def stage_send(idx, stage, unit, phase):
        guarded(roles(idx, stage, phase)[0], lambda: stage_copy(idx, stage, unit, phase).start())

    def stage_take(idx, stage, unit, phase):
        order = ORDERS[idx]
        first, rows = placed(phase)[idx]
        send_if, recv_if = roles(idx, stage, phase)
        ny, nz = landing_dims(order, stage)
        land, done = landings[idx, stage], order[:stage + 1]
        back = order[0] == 'w' and order[stage] == 'x'
        size = max(n for n in (128, 112, 96, 80, 64, 48, 32) if rows % n == 0)

        def take():
            stage_copy(idx, stage, unit, phase).wait_recv()
            for iy in range(ny):
                for iz in range(nz):
                    at_y = y if 'y' in done else iy
                    at_z = z if 'z' in done else iz

                    def chunk(k, carry):
                        offset = pl.multiple_of(k * size, 16)
                        here = (unit % N_SUM, at_y, at_z, pl.ds(first + offset, size), slice(None))
                        got = land[unit % SLOTS, iy, iz, pl.ds(offset, size), :]
                        big[here] = got if back else big[here] + got
                        return carry

                    lax.fori_loop(0, rows // size, chunk, 0)

        guarded(send_if, lambda: stage_copy(idx, stage, unit, phase).wait_send())
        guarded(recv_if, take)

    def part_list(phase):
        return [idx for idx in range(len(ORDERS)) if placed(phase)[idx][1]]

    def chip_sum(unit):
        d2d_copy(unit).wait()
        for iy in range(2):
            for iz in range(2):
                def chunk(k, carry):
                    here = pl.ds(pl.multiple_of(k * 128, 128), 128)
                    big[unit % N_SUM, iy, iz, here, :] = big[unit % N_SUM, iy, iz, here, :] + drecv[unit % 2, iy, iz, here, :]
                    return carry

                lax.fori_loop(0, 768 // 128, chunk, 0)
        for phase in range(2):
            @pl.when(unit // UNITS == phase)
            def _(phase=phase):
                for idx in part_list(phase):
                    stage_send(idx, 0, unit, phase)

    def finish(unit):
        sum_slot, pos = unit % N_SUM, unit % UNITS

        @pl.when((x == unit // UNITS) & (core == 0))
        def _():
            for j in range(6):
                out_ref[pl.ds(768 * pos + j, 128, stride=6), :] = big[sum_slot, y, z, pl.ds(128 * j, 128), :]

        @pl.when((x == unit // UNITS) & (core == 1))
        def _():
            for q in range(4):
                out_ref[pl.ds(6 * q + pos, 192, stride=24), :] = big[sum_slot, y, z, pl.ds(192 * q, 192), :]

    def due(tick, words):
        word = jnp.where(tick < 4 * STEPS, words[0], words[1])
        place = jnp.where(tick < 4 * STEPS, tick // 2, tick - 4 * STEPS)
        return (word >> place) & 1

    def run_ticks(tick, seen):
        now = []
        for place, (key, words) in enumerate(sorted(TAKES.items())):
            group, stage = key
            unit, bit = seen[place], due(tick, words)
            for phase in range(2):
                members = [i for i in (2 * group, 2 * group + 1) if placed(phase)[i][1]]
                if not members:
                    continue

                @pl.when((bit == 1) & (unit // UNITS == phase))
                def _(phase=phase, members=members, unit=unit, stage=stage):
                    for idx in members:
                        stage_take(idx, stage, unit, phase)
                        if stage + 1 < len(ORDERS[idx]):
                            stage_send(idx, stage + 1, unit, phase)
            now.append(unit + bit)
        unit, bit = seen[-1], due(tick, FINISH)

        @pl.when(bit == 1)
        def _():
            finish(unit)
        now.append(unit + bit)
        return tuple(now)

    def body(tick, seen):
        step, part = tick // 4, tick % 4
        live = step < STEPS

        @pl.when(live & (part == 0))
        def _():
            by_phase(step, wo_make, wait)

            def tile(t, c):
                rows = pl.ds(pl.multiple_of(t * TILE, TILE), TILE)
                h_v[rows, :] = hnew_v[rows, :]
                dh = lax.dot_general(dy_v[rows, :], wo_v[...], (((1,), (1,)), ((), ())), preferred_element_type=f32)
                dz_v[rows, :] = (dh * slope_v[rows, :]).astype(bf16)
                return c

            lax.fori_loop(0, ROWS // TILE, tile, 0)
            by_phase(step + 1, wo_make, start)
            by_phase(step + 1, z_make, wait)

        @pl.when(live & ((part == 1) | (part == 2)))
        def _():
            own = step % N_SUM
            is_a = (part == 1) == (core == 1)
            slot_a = jnp.where(core == 0, own, N_SUM)
            slot_b = jnp.where(core == 0, N_SUM, own)

            @pl.when(is_a)
            def _():
                def grad_a(nb, c):
                    cols = pl.ds(pl.multiple_of(nb * 256, 256), 256)
                    gelu_rows(nb * 384, 384)
                    total = None
                    for m in range(2):
                        rows = pl.ds(m * MICRO, MICRO)
                        got = lax.dot_general(h_v[rows, :], dy_v[rows, cols], (((0,), (0,)), ((), ())), preferred_element_type=f32)
                        got = got.astype(bf16).astype(f32)
                        total = got if total is None else total + got
                    for q in range(4):
                        for j in range(2):
                            here = pl.ds(pl.multiple_of((2 * nb + j) * 128, 128), 128)
                            big[slot_a, q // 2, q % 2, here, :] = total[128 * q:128 * q + 128, 128 * j:128 * j + 128]
                    return c

                lax.fori_loop(0, 3, grad_a, 0)

            @pl.when(jnp.logical_not(is_a))
            def _():
                @pl.when(step == 0)
                def _():
                    load_2.wait()

                @pl.when(step == UNITS)
                def _():
                    load_1.wait()

                def grad_b(nb, c):
                    cols = pl.ds(pl.multiple_of(nb * 256, 256), 256)
                    gelu_rows(1152 + nb * 448, 448)
                    total = None
                    for m in range(2):
                        rows = pl.ds(m * MICRO, MICRO)
                        got = lax.dot_general(x_v[rows, :], dz_v[rows, cols], (((0,), (0,)), ((), ())), preferred_element_type=f32)
                        got = got.astype(bf16).astype(f32)
                        total = got if total is None else total + got
                    for q in range(4):
                        for j in range(2):
                            here = pl.ds(pl.multiple_of((2 * nb + j) * 192, 64), 192)
                            big[slot_b, q // 2, q % 2, here, :] = total[192 * q:192 * q + 192, 128 * j:128 * j + 128]
                    return c

                lax.fori_loop(0, 2, grad_b, 0)

                @pl.when(step == UNITS - 1)
                def _():
                    load_1.start()

            @pl.when(part == 1)
            def _():
                d2d_copy(step).start()

            @pl.when(part == 2)
            def _():
                by_phase(step + 2, z_make, start)

        @pl.when((step < UNITS) & (part == 3))
        def _():
            for cp in wi_copies(step):
                cp.wait()

            def back(t, c):
                rows = pl.ds(pl.multiple_of(t * TILE, TILE), TILE)
                add = lax.dot_general(dz_v[rows, :], wi_v[...], (((1,), (1,)), ((), ())), preferred_element_type=f32)
                acc_v[rows, :] = jnp.where(step == 0, dy_v[rows, :].astype(f32), acc_v[rows, :]) + add
                return c

            lax.fori_loop(0, ROWS // TILE, back, 0)

            @pl.when(step < UNITS - 1)
            def _():
                for cp in wi_copies(step + 1):
                    cp.start()

            @pl.when(step == UNITS - 1)
            def _():
                def close(t, c):
                    rows = pl.ds(pl.multiple_of(t * 32, 32), 32)
                    dy_v[rows, :] = acc_v[rows, :].astype(bf16)
                    return c

                lax.fori_loop(0, ROWS // 32, close, 0)

        early = (part == 3) & (step < UNITS)
        late = (part == 0) & (step > UNITS) & (step <= STEPS)

        @pl.when(early | late)
        def _():
            chip_sum(jnp.where(part == 3, step, step - 1))

        return lax.cond((tick % 2 == 1) | (tick >= 4 * STEPS), lambda kept: run_ticks(tick, kept), lambda kept: kept, seen)

    lax.fori_loop(0, TICKS, body, (jnp.int32(0),) * (len(TAKES) + 1))


def solution(mesh):
    row_spec = P(('dz', 'dy', 'dx'), None)
    full_spec = P(None, None)

    def per_device(*arrays):
        f32, bf16 = jnp.float32, jnp.bfloat16
        landings = []
        for idx, stage in STAGES:
            ny, nz = landing_dims(ORDERS[idx], stage)
            landings.append(pltpu.VMEM((SLOTS, ny, nz, max(ROWS_ONE[idx], ROWS_TWO[idx]), 128), f32))
        out = pl.pallas_call(
            kernel,
            out_shape=jax.ShapeDtypeStruct((4608, 128), f32),
            in_specs=[pl.BlockSpec(memory_space=pl.ANY)] * 8,
            out_specs=pl.BlockSpec(memory_space=pltpu.VMEM),
            scratch_shapes=[
                pltpu.VMEM((ROWS, D), bf16),
                pltpu.VMEM((ROWS, D), bf16),
                pltpu.VMEM((ROWS, D), f32),
                pltpu.VMEM((ROWS, WIDE), bf16),
                pltpu.VMEM((ROWS, WIDE), bf16),
                pltpu.VMEM((ROWS, WIDE), bf16),
                pltpu.VMEM((ROWS, WIDE), f32),
                pltpu.VMEM((ROWS, WIDE), bf16),
                pltpu.VMEM((WIDE, D), bf16),
                pltpu.VMEM((D, WIDE), bf16),
                pltpu.VMEM((N_SUM + 1, 2, 2, 768, 128), f32),
                pltpu.VMEM((2, 2, 2, 768, 128), f32),
                *landings,
                pltpu.SemaphoreType.DMA((3,)),
                pltpu.SemaphoreType.DMA((4,)),
                pltpu.SemaphoreType.DMA((4,)),
                pltpu.SemaphoreType.DMA((4,)),
                pltpu.SemaphoreType.DMA((1,)),
                pltpu.SemaphoreType.DMA((2,)),
                pltpu.SemaphoreType.DMA((len(STAGES), SLOTS)),
                pltpu.SemaphoreType.DMA((len(STAGES), SLOTS)),
            ],
            compiler_params=pltpu.CompilerParams(collective_id=0, has_side_effects=True, vmem_limit_bytes=67043328),
        )(*arrays)
        return out.reshape(-1)

    return jax.shard_map(per_device, mesh=mesh, in_specs=(row_spec,) * 5 + (full_spec,) * 3, out_specs=P(('dx', 'dy', 'dz')), check_vma=False)
```

```python
import math

import jax
import jax.numpy as jnp
from jax import lax
from jax.experimental import pallas as pl
from jax.experimental.pallas import tpu as pltpu
from jax.sharding import PartitionSpec as P

MESH = pl.DeviceIdType.MESH
D = 768
FF = 3072
ROWS = 2048
MICRO = 1024
UNITS = 6
WIDE = 512
STEPS = 2 * UNITS
SLOTS = 6
TILE = 1024
ORDERS = ('yzx', 'zyx', 'xyz', 'xzy', 'wyzx', 'wzyx')
TAKES = {
    (0, 0): (5393064, 2114),
    (0, 1): (1348928, 172296),
    (0, 2): (595200, 1123356),
    (1, 0): (5589672, 66),
    (1, 1): (5393056, 37128),
    (1, 2): (1201408, 434440),
    (2, 0): (2381136, 17441),
    (2, 1): (2430272, 173058),
    (2, 2): (5313792, 951300),
    (2, 3): (1124352, 15743040),
}
FINISH = (1124352, 15743040)
N_SUM = 8
TICKS = 72
ROWS_ONE = (224, 224, 48, 48, 112, 112)
ROWS_TWO = (256, 256, 48, 48, 80, 80)
ROOT = math.sqrt(2.0 / math.pi)
CUBE = 0.044715


def gelu_pair(val):
    sq = val * val
    tan = jnp.tanh(val * (sq * (ROOT * CUBE) + ROOT))
    cdf = 0.5 * tan + 0.5
    bump = val * (cdf * (1.0 - cdf))
    return val * cdf, cdf + bump * (sq * (6.0 * ROOT * CUBE) + 2.0 * ROOT)


def landing_dims(order, stage):
    done = order[:stage + 1]
    return (1 if 'y' in done else 2), (1 if 'z' in done else 2)


def stage_list():
    return [(idx, stage) for idx, order in enumerate(ORDERS) for stage in range(len(order))]


STAGES = stage_list()


def kernel(a1_hbm, z1_hbm, a2_hbm, z2_hbm, g_hbm, wi_hbm, wo1_hbm, wo2_hbm, out_ref,
           dy_v, x_v, acc_v, z_v, hnew_v, h_v, slope_v, dz_v, wo_v, wi_v, big, drecv, *rest):
    landings = dict(zip(STAGES, rest[:len(STAGES)]))
    isem, zsem, osem, wsem, dsend_sem, drecv_sem, send_sem, recv_sem = rest[len(STAGES):]
    f32, bf16 = jnp.float32, jnp.bfloat16
    dx, y, z = lax.axis_index('dx'), lax.axis_index('dy'), lax.axis_index('dz')
    x, core = dx // 2, dx % 2
    peers = {'x': {'dx': (dx + 2) % 4}, 'y': {'dy': 1 - y}, 'z': {'dz': 1 - z}, 'c': {'dx': dx + 1 - 2 * core}}
    peers['w'] = peers['x']

    barrier = pltpu.get_barrier_semaphore()
    for name in 'xyzc':
        pl.semaphore_signal(barrier, inc=1, device_id=peers[name], device_id_type=MESH)

    load_g = pltpu.make_async_copy(g_hbm, dy_v, isem.at[0])
    load_2 = pltpu.make_async_copy(a2_hbm, x_v, isem.at[1])
    load_1 = pltpu.make_async_copy(a1_hbm, x_v, isem.at[2])

    def columns(unit, quarter):
        return pl.ds(pl.multiple_of(quarter * 768 + unit * 128, 128), 128), pl.ds(quarter * 128, 128)

    def z_copies(unit, hbm):
        pairs = [columns(unit, q) for q in range(4)]
        return [pltpu.make_async_copy(hbm.at[:, get], z_v.at[:, put], zsem.at[q]) for q, (get, put) in enumerate(pairs)]

    def wo_copies(unit, hbm):
        pairs = [columns(unit, q) for q in range(4)]
        return [pltpu.make_async_copy(hbm.at[get, :], wo_v.at[put, :], osem.at[q]) for q, (get, put) in enumerate(pairs)]

    def wi_copies(unit):
        pairs = [columns(unit, q) for q in range(4)]
        return [pltpu.make_async_copy(wi_hbm.at[:, get], wi_v.at[:, put], wsem.at[q]) for q, (get, put) in enumerate(pairs)]

    def by_phase(step, make, action):
        @pl.when(step < UNITS)
        def _():
            for cp in make(step, 0):
                action(cp)

        @pl.when((step >= UNITS) & (step < STEPS))
        def _():
            for cp in make(step - UNITS, 1):
                action(cp)

    def z_make(unit, phase):
        return z_copies(unit, z1_hbm if phase else z2_hbm)

    def wo_make(unit, phase):
        return wo_copies(unit, wo1_hbm if phase else wo2_hbm)

    def start(cp):
        cp.start()

    def wait(cp):
        cp.wait()

    for cp in z_copies(0, z2_hbm):
        cp.start()
    for cp in wo_copies(0, wo2_hbm):
        cp.start()
    load_g.start()
    load_2.start()
    for cp in wi_copies(0):
        cp.start()

    def gelu_rows(start, count):
        for k in range(count // 32):
            rows = pl.ds(pl.multiple_of(start + k * 32, 32), 32)
            hid, slope = gelu_pair(z_v[rows, :].astype(f32))
            hnew_v[rows, :] = hid.astype(bf16)
            slope_v[rows, :] = slope

    for cp in z_copies(0, z2_hbm):
        cp.wait()

    def first_gelu(t, c):
        gelu_rows(t * 128, 128)
        return c

    lax.fori_loop(0, ROWS // 128, first_gelu, 0)
    for cp in z_copies(1, z2_hbm):
        cp.start()
    load_g.wait()
    pl.semaphore_wait(barrier, 4)

    def d2d_copy(unit):
        return pltpu.make_async_remote_copy(src_ref=big.at[N_SUM], dst_ref=drecv.at[unit % 2], send_sem=dsend_sem.at[0],
                                            recv_sem=drecv_sem.at[unit % 2], device_id=peers['c'], device_id_type=MESH)

    def placed(phase):
        sizes = (ROWS_ONE, ROWS_TWO)[phase]
        starts = [sum(sizes[:k]) for k in range(len(sizes))]
        return list(zip(starts, sizes))

    def stage_copy(idx, stage, unit, phase):
        order = ORDERS[idx]
        first, rows = placed(phase)[idx]
        done, axis = order[:stage], order[stage]
        at_y = pl.ds(1 - y, 1) if axis == 'y' else pl.ds(y, 1) if 'y' in done else pl.ds(0, 2)
        at_z = pl.ds(1 - z, 1) if axis == 'z' else pl.ds(z, 1) if 'z' in done else pl.ds(0, 2)
        slot, sem = unit % SLOTS, STAGES.index((idx, stage))
        return pltpu.make_async_remote_copy(src_ref=big.at[unit % N_SUM, at_y, at_z, pl.ds(first, rows), :],
                                            dst_ref=landings[idx, stage].at[slot, :, :, pl.ds(0, rows), :],
                                            send_sem=send_sem.at[sem, slot], recv_sem=recv_sem.at[sem, slot],
                                            device_id=peers[axis], device_id_type=MESH)

    def roles(idx, stage, phase):
        order = ORDERS[idx]
        if order[stage] == 'w':
            return x == phase, x != phase
        if order[stage] == 'x':
            return x != phase, x == phase
        done = order[:stage]
        if 'x' in done:
            return x == phase, x == phase
        if 'w' in done:
            return x != phase, x != phase
        return None, None

    def guarded(cond, body):
        if cond is None:
            body()
        else:
            pl.when(cond)(body)

    def stage_send(idx, stage, unit, phase):
        guarded(roles(idx, stage, phase)[0], lambda: stage_copy(idx, stage, unit, phase).start())

    def stage_take(idx, stage, unit, phase):
        order = ORDERS[idx]
        first, rows = placed(phase)[idx]
        send_if, recv_if = roles(idx, stage, phase)
        ny, nz = landing_dims(order, stage)
        land, done = landings[idx, stage], order[:stage + 1]
        back = order[0] == 'w' and order[stage] == 'x'
        size = max(n for n in (128, 112, 96, 80, 64, 48, 32) if rows % n == 0)

        def take():
            stage_copy(idx, stage, unit, phase).wait_recv()
            for iy in range(ny):
                for iz in range(nz):
                    at_y = y if 'y' in done else iy
                    at_z = z if 'z' in done else iz

                    def chunk(k, carry):
                        offset = pl.multiple_of(k * size, 16)
                        here = (unit % N_SUM, at_y, at_z, pl.ds(first + offset, size), slice(None))
                        got = land[unit % SLOTS, iy, iz, pl.ds(offset, size), :]
                        big[here] = got if back else big[here] + got
                        return carry

                    lax.fori_loop(0, rows // size, chunk, 0)

        guarded(send_if, lambda: stage_copy(idx, stage, unit, phase).wait_send())
        guarded(recv_if, take)

    def part_list(phase):
        return [idx for idx in range(len(ORDERS)) if placed(phase)[idx][1]]

    def chip_sum(unit):
        d2d_copy(unit).wait()
        for iy in range(2):
            for iz in range(2):
                def chunk(k, carry):
                    here = pl.ds(pl.multiple_of(k * 128, 128), 128)
                    big[unit % N_SUM, iy, iz, here, :] = big[unit % N_SUM, iy, iz, here, :] + drecv[unit % 2, iy, iz, here, :]
                    return carry

                lax.fori_loop(0, 768 // 128, chunk, 0)
        for phase in range(2):
            @pl.when(unit // UNITS == phase)
            def _(phase=phase):
                for idx in part_list(phase):
                    stage_send(idx, 0, unit, phase)

    def finish(unit):
        sum_slot, pos = unit % N_SUM, unit % UNITS

        @pl.when((x == unit // UNITS) & (core == 0))
        def _():
            for j in range(6):
                out_ref[pl.ds(768 * pos + j, 128, stride=6), :] = big[sum_slot, y, z, pl.ds(128 * j, 128), :]

        @pl.when((x == unit // UNITS) & (core == 1))
        def _():
            for q in range(4):
                out_ref[pl.ds(6 * q + pos, 192, stride=24), :] = big[sum_slot, y, z, pl.ds(192 * q, 192), :]

    def due(tick, words):
        word = jnp.where(tick < 4 * STEPS, words[0], words[1])
        place = jnp.where(tick < 4 * STEPS, tick // 2, tick - 4 * STEPS)
        return (word >> place) & 1

    def run_ticks(tick, seen):
        now = []
        for place, (key, words) in enumerate(sorted(TAKES.items())):
            group, stage = key
            unit, bit = seen[place], due(tick, words)
            for phase in range(2):
                members = [i for i in (2 * group, 2 * group + 1) if placed(phase)[i][1]]
                if not members:
                    continue

                @pl.when((bit == 1) & (unit // UNITS == phase))
                def _(phase=phase, members=members, unit=unit, stage=stage):
                    for idx in members:
                        stage_take(idx, stage, unit, phase)
                        if stage + 1 < len(ORDERS[idx]):
                            stage_send(idx, stage + 1, unit, phase)
            now.append(unit + bit)
        unit, bit = seen[-1], due(tick, FINISH)

        @pl.when(bit == 1)
        def _():
            finish(unit)
        now.append(unit + bit)
        return tuple(now)

    def body(tick, seen):
        step, part = tick // 4, tick % 4
        live = step < STEPS

        @pl.when(live & (part == 0))
        def _():
            by_phase(step, wo_make, wait)

            def tile(t, c):
                rows = pl.ds(pl.multiple_of(t * TILE, TILE), TILE)
                h_v[rows, :] = hnew_v[rows, :]
                dh = lax.dot_general(dy_v[rows, :], wo_v[...], (((1,), (1,)), ((), ())), preferred_element_type=f32)
                dz_v[rows, :] = (dh * slope_v[rows, :]).astype(bf16)
                return c

            lax.fori_loop(0, ROWS // TILE, tile, 0)
            by_phase(step + 1, wo_make, start)
            by_phase(step + 1, z_make, wait)

        @pl.when(live & ((part == 1) | (part == 2)))
        def _():
            own = step % N_SUM
            is_a = (part == 1) == (core == 1)
            slot_a = jnp.where(core == 0, own, N_SUM)
            slot_b = jnp.where(core == 0, N_SUM, own)

            @pl.when(is_a)
            def _():
                def grad_a(nb, c):
                    cols = pl.ds(pl.multiple_of(nb * 256, 256), 256)
                    gelu_rows(nb * 384, 384)
                    total = None
                    for m in range(2):
                        rows = pl.ds(m * MICRO, MICRO)
                        got = lax.dot_general(h_v[rows, :], dy_v[rows, cols], (((0,), (0,)), ((), ())), preferred_element_type=f32)
                        got = got.astype(bf16).astype(f32)
                        total = got if total is None else total + got
                    for q in range(4):
                        for j in range(2):
                            here = pl.ds(pl.multiple_of((2 * nb + j) * 128, 128), 128)
                            big[slot_a, q // 2, q % 2, here, :] = total[128 * q:128 * q + 128, 128 * j:128 * j + 128]
                    return c

                lax.fori_loop(0, 3, grad_a, 0)

            @pl.when(jnp.logical_not(is_a))
            def _():
                @pl.when(step == 0)
                def _():
                    load_2.wait()

                @pl.when(step == UNITS)
                def _():
                    load_1.wait()

                def grad_b(nb, c):
                    cols = pl.ds(pl.multiple_of(nb * 256, 256), 256)
                    gelu_rows(1152 + nb * 448, 448)
                    total = None
                    for m in range(2):
                        rows = pl.ds(m * MICRO, MICRO)
                        got = lax.dot_general(x_v[rows, :], dz_v[rows, cols], (((0,), (0,)), ((), ())), preferred_element_type=f32)
                        got = got.astype(bf16).astype(f32)
                        total = got if total is None else total + got
                    for q in range(4):
                        for j in range(2):
                            here = pl.ds(pl.multiple_of((2 * nb + j) * 192, 64), 192)
                            big[slot_b, q // 2, q % 2, here, :] = total[192 * q:192 * q + 192, 128 * j:128 * j + 128]
                    return c

                lax.fori_loop(0, 2, grad_b, 0)

                @pl.when(step == UNITS - 1)
                def _():
                    load_1.start()

            @pl.when(part == 1)
            def _():
                d2d_copy(step).start()

            @pl.when(part == 2)
            def _():
                by_phase(step + 2, z_make, start)

        @pl.when((step < UNITS) & (part == 3))
        def _():
            for cp in wi_copies(step):
                cp.wait()

            def back(t, c):
                rows = pl.ds(pl.multiple_of(t * TILE, TILE), TILE)
                add = lax.dot_general(dz_v[rows, :], wi_v[...], (((1,), (1,)), ((), ())), preferred_element_type=f32)
                acc_v[rows, :] = jnp.where(step == 0, dy_v[rows, :].astype(f32), acc_v[rows, :]) + add
                return c

            lax.fori_loop(0, ROWS // TILE, back, 0)

            @pl.when(step < UNITS - 1)
            def _():
                for cp in wi_copies(step + 1):
                    cp.start()

            @pl.when(step == UNITS - 1)
            def _():
                def close(t, c):
                    rows = pl.ds(pl.multiple_of(t * 32, 32), 32)
                    dy_v[rows, :] = acc_v[rows, :].astype(bf16)
                    return c

                lax.fori_loop(0, ROWS // 32, close, 0)

        early = (part == 3) & (step < UNITS)
        late = (part == 0) & (step > UNITS) & (step <= STEPS)

        @pl.when(early | late)
        def _():
            chip_sum(jnp.where(part == 3, step, step - 1))

        return lax.cond((tick % 2 == 1) | (tick >= 4 * STEPS), lambda kept: run_ticks(tick, kept), lambda kept: kept, seen)

    lax.fori_loop(0, TICKS, body, (jnp.int32(0),) * (len(TAKES) + 1))


def solution(mesh):
    row_spec = P(('dz', 'dy', 'dx'), None)
    full_spec = P(None, None)

    def per_device(*arrays):
        f32, bf16 = jnp.float32, jnp.bfloat16
        landings = []
        for idx, stage in STAGES:
            ny, nz = landing_dims(ORDERS[idx], stage)
            landings.append(pltpu.VMEM((SLOTS, ny, nz, max(ROWS_ONE[idx], ROWS_TWO[idx]), 128), f32))
        out = pl.pallas_call(
            kernel,
            out_shape=jax.ShapeDtypeStruct((4608, 128), f32),
            in_specs=[pl.BlockSpec(memory_space=pl.ANY)] * 8,
            out_specs=pl.BlockSpec(memory_space=pltpu.VMEM),
            scratch_shapes=[
                pltpu.VMEM((ROWS, D), bf16),
                pltpu.VMEM((ROWS, D), bf16),
                pltpu.VMEM((ROWS, D), f32),
                pltpu.VMEM((ROWS, WIDE), bf16),
                pltpu.VMEM((ROWS, WIDE), bf16),
                pltpu.VMEM((ROWS, WIDE), bf16),
                pltpu.VMEM((ROWS, WIDE), f32),
                pltpu.VMEM((ROWS, WIDE), bf16),
                pltpu.VMEM((WIDE, D), bf16),
                pltpu.VMEM((D, WIDE), bf16),
                pltpu.VMEM((N_SUM + 1, 2, 2, 768, 128), f32),
                pltpu.VMEM((2, 2, 2, 768, 128), f32),
                *landings,
                pltpu.SemaphoreType.DMA((3,)),
                pltpu.SemaphoreType.DMA((4,)),
                pltpu.SemaphoreType.DMA((4,)),
                pltpu.SemaphoreType.DMA((4,)),
                pltpu.SemaphoreType.DMA((1,)),
                pltpu.SemaphoreType.DMA((2,)),
                pltpu.SemaphoreType.DMA((len(STAGES), SLOTS)),
                pltpu.SemaphoreType.DMA((len(STAGES), SLOTS)),
            ],
            compiler_params=pltpu.CompilerParams(collective_id=0, has_side_effects=True, vmem_limit_bytes=67043328),
        )(*arrays)
        return out.reshape(-1)

    return jax.shard_map(per_device, mesh=mesh, in_specs=(row_spec,) * 5 + (full_spec,) * 3, out_specs=P(('dx', 'dy', 'dz')), check_vma=False)
```
